32 devices in a mesh: row: 8 (over z, x), col: 4 (over y, core).
Axes of the slice: x: 2, y: 2, z: 4, core: 2. Of those that a mesh axis runs over, the one named last changes fastest.
Arguments:
- sparse_blocks: float32 [4096, 128, 128], P(('row', 'col')), may hold values from -0.5 to 0.5
- panel_rows: float32 [262144, 128], P(('row', 'col')), may hold values from -6 to 6
- block_row: int32 [4096], P(('row', 'col')), may hold values from 0 to 63
- block_owner: int32 [4096, 1], P(('row', 'col')), may hold values from 0 to 31; in each aligned block of 128 rows (0 to 127, 128 to 255, ...) at most 8 rows name the same one
- block_offset: int32 [4096], P(('row', 'col')), may hold values from 0 to 63
Outputs:
- result: float32 [262144, 128], P(('row', 'col'))
The draws below stay inside these ranges and needn't reach their ends.
Inputs may be any that keep to these rules, and one draw needn't show every extreme that they name: `block_owner`: among the blocks of one device, at most 8 name the same owner, a bound that some block reaches.
All inputs are finite; a program needn't handle non-finite values.
Results may differ from the reference program's by a relative error of at most 0.0001.
Values sent between devices are 32-bit elements; how exact they have to be, the bound alone decides.
A program may use at most 192 MiB of HBM per device.

```python
import math
import jax
import jax.numpy as jnp
import numpy as np
from jax import lax

BLK = 128
PANEL = 128
RB_DEV = 64
SLOTS = 128
CAP = 8
NB = 2048
NNZ = 4096
N_ROW = 8
N_COL = 4


def plant(array, rng, smallest, top_value):
    index_at = [jax.random.randint(jax.random.fold_in(rng, axis), (), 0, length) for axis, length in enumerate(array.shape)]
    widest = array.shape.index(max(array.shape))
    beside = index_at[:widest] + [(index_at[widest] + 1) % array.shape[widest]] + index_at[widest + 1:]
    return array.at[tuple(index_at)].set(smallest).at[tuple(beside)].set(top_value)


def steps_of(key, shape, pieces, low, top_value):
    gain, own = 1.0, jax.random.fold_in(key, 6)
    for position, shards_of in pieces:
        draws = jnp.exp(jax.random.uniform(jax.random.fold_in(own, position), (shards_of,), jnp.float32, low / len(pieces), top_value / len(pieces)))
        gain = gain * jnp.repeat(draws, shape[position] // shards_of).reshape([-1 if axis == position else 1 for axis in range(len(shape))])
    return gain


def rank_table(number_of, lean):
    weights = [(1 << 20) // math.isqrt(rank ** lean) + 1 for rank in range(1, number_of + 1)]
    scale = 1 + sum(weights) // (1 << 30)
    return np.cumsum(np.array([max(1, weight // scale) for weight in weights]))


def ranked_ids(stream_key, extent, count, slope):
    listing = rank_table(count, slope)
    ticket = jax.random.randint(jax.random.fold_in(stream_key, 1), extent, 0, int(listing[count - 1]))
    standing = jnp.searchsorted(jnp.asarray(listing, jnp.int32), ticket, side="right")
    return jax.random.permutation(jax.random.fold_in(stream_key, 2), count)[standing].astype(jnp.int32)


def deal_out(stream_key, own, number, rows, number_of, top, limit, skew):
    sequence = jax.random.permutation(stream_key, number_of)
    heavy_load, common = shares(number_of, rows * top, limit, skew, True), shares(number_of, rows * top, limit, skew, False)
    places = jnp.arange(number_of)

    def named(lengths, offset_by):
        used = int((lengths > 0).sum())
        fixed = max(1, used // 4)
        moved = fixed + (places - fixed + offset_by * (used - fixed)) % max(1, number_of - fixed)
        return jnp.zeros((number_of,), jnp.int32).at[sequence[jnp.where(places < fixed, places, moved)]].set(jnp.asarray(lengths, jnp.int32))

    lengths = jnp.where(number % 4 == 0, named(heavy_load, number // 4), named(common, number - number // 4 - 1))
    mixed = jax.random.permutation(jax.random.fold_in(own, 3), number_of)
    source_of, sink = mixed[0:number_of // 2 * 2:2], mixed[1:number_of // 2 * 2:2]
    slack = jnp.minimum(lengths[source_of] - 1, limit - lengths[sink]) // 2
    slack = jnp.where((source_of == sequence[0]) | (sink == sequence[0]) | (lengths[sink] == 0), 0, jnp.maximum(slack, 0))
    moved = jax.random.randint(jax.random.fold_in(own, 4), (number_of // 2,), 0, 1 << 20) % (slack + 1)
    lengths = lengths.at[source_of].add(-moved).at[sink].add(moved)
    items = jnp.searchsorted(jnp.cumsum(lengths), jnp.arange(rows * top), side="right").astype(jnp.int32)
    table = items.reshape(top, rows).T
    table = table[jax.random.permutation(jax.random.fold_in(own, 1), rows)]
    offset_by = jax.random.randint(jax.random.fold_in(own, 2), (rows, 1), 0, top)
    return jnp.take_along_axis(table, (jnp.arange(top)[None, :] + offset_by) % top, axis=1)


def shares(number_of, total, limit, lean, full):
    loads = [(1 << 20) // math.isqrt(rank ** lean) + 1 for rank in range(1, number_of + 1)]
    largest = limit if full else min(limit, max(-(-total // number_of), total * loads[0] // sum(loads)))
    least = 1 if total - largest >= number_of - 1 else 0
    given, surplus = [largest] + [least] * (number_of - 1), total - largest - least * (number_of - 1)
    while surplus > 0:
        movable = [i for i in range(1, number_of) if given[i] < largest] or [i for i in range(1, number_of) if given[i] < limit]
        pool, remaining = sum([loads[i] for i in movable]), surplus
        for i in movable:
            more = min(limit - given[i], max(1, remaining * loads[i] // pool), surplus)
            given[i] = given[i] + more
            surplus = surplus - more
    return np.array(given)


def noise(rng, dims, deviation, reach, pieces=(), kind=jnp.bfloat16):
    values = deviation * jax.random.normal(rng, dims, jnp.float32)
    if pieces:
        values = values * steps_of(rng, dims, pieces, -0.22, 0.18)
    return jnp.clip(values, -reach, reach).astype(kind)


def setup_inputs(seed: int = 0) -> dict:
    keys = jax.random.split(jax.random.key(seed), 6)
    sparse_blocks = noise(keys[0], (NNZ, BLK, BLK), BLK ** -0.5, 0.5, ((0, 32),), jnp.float32)
    panel_rows = noise(keys[1], (NB * BLK, PANEL), 1.0, 6.0, ((0, 32),), jnp.float32)
    block_row = plant(ranked_ids(keys[2], (NNZ,), RB_DEV, 2), jax.random.fold_in(keys[2], 3), 0, RB_DEV - 1).astype(jnp.int32)
    block_owner_keys = jax.random.split(jax.random.fold_in(keys[3], 1), NNZ // SLOTS)
    block_owner_turns = jax.random.permutation(jax.random.fold_in(keys[3], 3), NNZ // SLOTS)
    block_owner = jax.vmap(lambda own, number: deal_out(jax.random.fold_in(keys[3], 2), own, number, SLOTS, N_ROW * N_COL, 1, CAP, 2))(block_owner_keys, block_owner_turns).reshape((NNZ, 1))
    block_offset = plant(jax.random.randint(keys[4], (NNZ,), 0, RB_DEV), jax.random.fold_in(keys[4], 1), 0, RB_DEV - 1).astype(jnp.int32)
    return {"sparse_blocks": sparse_blocks, "panel_rows": panel_rows, "block_row": block_row, "block_owner": block_owner, "block_offset": block_offset}


def reference(sparse_blocks, panel_rows, block_row, block_owner, block_offset):
    device_count = N_ROW * N_COL
    panel_blocks = panel_rows.reshape(device_count * RB_DEV, BLK, PANEL)
    owners = block_owner[:, 0]

    def advance(device_index, accum):
        device_index = device_index.astype(jnp.int32)
        start = device_index * SLOTS
        piece_a = lax.dynamic_slice_in_dim(sparse_blocks, start, SLOTS, 0)
        row_ids = (lax.dynamic_slice_in_dim(block_row, start, SLOTS, 0) + device_index * RB_DEV).astype(jnp.int32)
        col_ids = (lax.dynamic_slice_in_dim(owners, start, SLOTS, 0) * RB_DEV + lax.dynamic_slice_in_dim(block_offset, start, SLOTS, 0)).astype(jnp.int32)
        products = jnp.einsum("sij,sik->sjk", piece_a, panel_blocks[row_ids], precision=lax.Precision.HIGHEST)
        return accum.at[col_ids].add(products)

    accum = lax.fori_loop(0, device_count, advance, jnp.zeros((device_count * RB_DEV, BLK, PANEL), jnp.float32))
    return accum.reshape(device_count * RB_DEV * BLK, PANEL)
```

```python
import functools

import jax
import jax.numpy as jnp
from jax import lax
from jax.experimental import pallas as pl
from jax.experimental.pallas import tpu as pltpu
from jax.sharding import PartitionSpec as P

AXES = ("row", "col")
VMEM_LIMIT = 67_000_000
LANES = 128
TILE = 8
MESH = pl.DeviceIdType.MESH


def split_parts(value):
    high = value.astype(jnp.bfloat16)
    low = (value - high.astype(jnp.float32)).astype(jnp.bfloat16)
    return high, low


def block_product(block, panel):
    block_high, block_low = split_parts(block)
    panel_high, panel_low = split_parts(panel)
    dims = (((0,), (0,)), ((), ()))
    dot = functools.partial(lax.dot_general, dimension_numbers=dims, preferred_element_type=jnp.float32)
    return dot(
        jnp.concatenate([block_high, block_low], axis=0),
        jnp.concatenate([panel_high, panel_high], axis=0),
    ) + dot(block_high, panel_low)


def peers_of(upper, lower, outer):
    moves = [
        (a, b, c) for a in range(upper) for b in range(lower) for c in range(outer) if (a, b, c) != (0, 0, 0)
    ]
    single = [move for move in moves if sum(digit > 0 for digit in move) == 1]
    double = [move for move in moves if sum(digit > 0 for digit in move) == 2]
    zeros = lambda move: tuple(digit == 0 for digit in move)
    order = sorted(single, key=zeros)
    opposite = sorted(double, key=lambda move: tuple(digit > 0 for digit in move))
    pairs = list(zip(order, opposite))
    first = [one for one, _ in pairs] + [other for _, other in pairs]
    second = [other for _, other in pairs] + [one for one, _ in pairs]
    rest = [move for move in moves if move not in first]
    return first + rest, second + rest


def route_kernel(
    row_half,
    per_owner,
    source_ref,
    panel_at_ref,
    keep_ref,
    sparse_hbm,
    panel_hbm,
    table_hbm,
    out_hbm,
    sparse,
    panel,
    products,
    far_land,
    near_land,
    sums,
    crossed,
    total,
    tables,
    near_table,
    far_table,
    data_send,
    data_recv,
    table_send,
    table_recv,
    cross_send,
    cross_recv,
    load_sems,
    own_sems,
    out_sems,
):
    row, col = lax.axis_index("row"), lax.axis_index("col")
    row_count, col_count = lax.axis_size("row"), lax.axis_size("col")
    half, inner = row // row_half, row % row_half
    outer, core = col // 2, col % 2
    lower = min(2, row_half)
    mine = inner * col_count + col
    count = row_half * col_count
    half_slots = count * per_owner
    upper_count, outer_count = row_half // lower, col_count // 2
    local_blocks = total.shape[0]
    chunk = min(8, local_blocks)
    chunks = local_blocks // chunk

    loads = [
        pltpu.make_async_copy(sparse_hbm, sparse, load_sems.at[0]),
        pltpu.make_async_copy(panel_hbm, panel, load_sems.at[1]),
    ]
    for load in loads:
        load.start()
    blank = jnp.zeros(far_land.shape[1:], jnp.float32)
    far_land[half_slots] = blank
    near_land[half_slots] = blank

    def target(move_pair, flip):
        one, other = move_pair
        a, b, c = (x + core * (y - x) for x, y in zip(one, other))
        there = (inner // lower + a) % upper_count * lower + (inner % lower + b) % lower
        beside = (outer + c) % outer_count * 2 + (core + flip) % 2
        number = ((a * lower + b) * outer_count + c) * 2 + flip
        return (half * row_half + there, beside), there * col_count + beside, number

    firsts, seconds = peers_of(upper_count, lower, outer_count)
    moves = list(zip(firsts, seconds))
    still = ((0, 0, 0), (0, 0, 0))
    targets = [target(move, (core + phase) % 2) for phase in range(2) for move in moves]
    targets.append(target(still, 1))
    opposite = ((row + row_half) % row_count, col)

    barrier = pltpu.get_barrier_semaphore()
    for device, _, _ in targets:
        pl.semaphore_signal(barrier, inc=1, device_id=device, device_id_type=MESH)
    pl.semaphore_signal(barrier, inc=1, device_id=opposite, device_id_type=MESH)
    pl.semaphore_wait(barrier, len(targets) + 1)

    def remote(source, destination, send_sem, recv_sem, device):
        copy = pltpu.make_async_remote_copy(
            src_ref=source,
            dst_ref=destination,
            send_sem=send_sem,
            recv_sem=recv_sem,
            device_id=device,
            device_id_type=MESH,
        )
        copy.start()
        return copy

    table_copies = [
        remote(table_hbm.at[place], tables.at[mine], table_send.at[number], table_recv.at[number], device)
        for device, place, number in targets
    ]
    own_table = pltpu.make_async_copy(table_hbm.at[mine], tables.at[mine], own_sems.at[0])
    own_table.start()
    for load in loads:
        load.wait()

    unit = min(4, per_owner)

    def fill(base, place, destination, at):
        first = base + place * per_owner

        def some(step, _):
            for k in range(unit):
                slot = step * unit + k
                source = source_ref[first + slot]
                product = block_product(sparse[source], panel[panel_at_ref[first + slot]])
                before = destination[at + jnp.maximum(slot - 1, 0)]
                product = product + jnp.where(keep_ref[first + slot] > 0, before, 0.0)
                destination[at + slot] = product
            return 0

        lax.fori_loop(0, per_owner // unit, some, 0)

    def spread(base, land, shift):
        copies = []
        for device, place, number in targets:
            at = base + place * per_owner
            fill(base, place, products, at)
            copies.append(
                remote(
                    products.at[pl.ds(at, per_owner)],
                    land.at[pl.ds(mine * per_owner, per_owner)],
                    data_send.at[shift + number],
                    data_recv.at[shift + number],
                    device,
                )
            )
        fill(base, mine, land, mine * per_owner)
        return copies

    far_copies = spread(half_slots, far_land, count)
    near_copies = spread(0, near_land, 0)

    own_table.wait()
    for copy in table_copies:
        copy.wait_recv()
    lookups = [
        pltpu.make_async_copy(tables.at[:, 0, :], near_table, own_sems.at[1]),
        pltpu.make_async_copy(tables.at[:, TILE, :], far_table, own_sems.at[2]),
    ]
    for lookup in lookups:
        lookup.start()
    for lookup in lookups:
        lookup.wait()

    def reduce(land, table, destination, first, number):
        def one(step, _):
            column = first + step
            value = land[table[0, column]]
            for origin in range(1, count):
                value = value + land[table[origin, column]]
            destination[column] = value
            return 0

        lax.fori_loop(0, number, one, 0)

    for copy in far_copies:
        copy.wait_recv()
    cross_copies = []
    for index in range(chunks):
        reduce(far_land, far_table, sums, index * chunk, chunk)
        part = pl.ds(index * chunk, chunk)
        cross_copies.append(
            remote(sums.at[part], crossed.at[part], cross_send.at[index], cross_recv.at[index], opposite)
        )
    for copy in near_copies:
        copy.wait_recv()
    reduce(near_land, near_table, total, 0, local_blocks)
    outs = []
    for index, copy in enumerate(cross_copies):
        copy.wait_recv()
        part = pl.ds(index * chunk, chunk)
        total[part] = total[part] + crossed[part]
        out = pltpu.make_async_copy(total.at[part], out_hbm.at[part], out_sems.at[index])
        out.start()
        outs.append(out)
    for copy in table_copies + far_copies + near_copies + cross_copies:
        copy.wait_send()
    for out in outs:
        out.wait()


def route(source, panel_at, keep, sparse_blocks, panel_blocks, table, row_half, per_owner):
    count = row_half * lax.axis_size("col")
    local_blocks, size, width = panel_blocks.shape
    half_slots = count * per_owner
    chunks = local_blocks // min(8, local_blocks)
    lanes = table.shape[-1]
    scalars = pl.BlockSpec(memory_space=pltpu.SMEM)
    anywhere = pl.BlockSpec(memory_space=pl.ANY)
    block = (size, width)
    dma = pltpu.SemaphoreType.DMA
    return pl.pallas_call(
        functools.partial(route_kernel, row_half, per_owner),
        in_specs=[scalars] * 3 + [anywhere] * 3,
        out_specs=anywhere,
        out_shape=jax.ShapeDtypeStruct((local_blocks,) + block, jnp.float32),
        scratch_shapes=[
            pltpu.VMEM(sparse_blocks.shape, jnp.float32),
            pltpu.VMEM(panel_blocks.shape, jnp.float32),
            pltpu.VMEM((2 * half_slots,) + block, jnp.float32),
            pltpu.VMEM((half_slots + 1,) + block, jnp.float32),
            pltpu.VMEM((half_slots + 1,) + block, jnp.float32),
            pltpu.VMEM((local_blocks,) + block, jnp.float32),
            pltpu.VMEM((local_blocks,) + block, jnp.float32),
            pltpu.VMEM((local_blocks,) + block, jnp.float32),
            pltpu.VMEM((count, 2 * TILE, lanes), jnp.int32),
            pltpu.SMEM((count, lanes), jnp.int32),
            pltpu.SMEM((count, lanes), jnp.int32),
            dma((2 * count,)),
            dma((2 * count,)),
            dma((count,)),
            dma((count,)),
            dma((chunks,)),
            dma((chunks,)),
            dma((2,)),
            dma((3,)),
            dma((chunks,)),
        ],
        compiler_params=pltpu.CompilerParams(
            collective_id=0, has_side_effects=True, vmem_limit_bytes=VMEM_LIMIT
        ),
    )(source, panel_at, keep, sparse_blocks, panel_blocks, table)


def body(sparse_blocks, panel_rows, block_row, block_owner, block_offset):
    device_count = lax.axis_size("row") * lax.axis_size("col")
    half_count = device_count // 2
    slot_count, size, _ = sparse_blocks.shape
    width = panel_rows.shape[1]
    local_blocks = panel_rows.shape[0] // size
    per_owner = max(2, 2 * slot_count // device_count)
    half_slots = half_count * per_owner
    me = lax.axis_index(AXES)
    my_half = me // half_count
    row_half = lax.axis_size("row") // 2
    owner = block_owner[:, 0]
    index = jnp.arange(slot_count, dtype=jnp.int32)
    key = block_offset * slot_count + index
    same = owner[:, None] == owner[None, :]
    earlier = same & (key[None, :] < key[:, None])
    order = jnp.sum(earlier.astype(jnp.int32), axis=1)
    again = jnp.any(earlier & (block_offset[None, :] == block_offset[:, None]), axis=1).astype(jnp.int32)
    half_of = (owner // half_count != my_half).astype(jnp.int32)
    group = half_of * half_count + owner % half_count
    position = group * per_owner + order
    hit = position[None, :] == jnp.arange(2 * half_slots, dtype=jnp.int32)[:, None]
    pick = lambda value: jnp.max(jnp.where(hit, value[None, :], 0), axis=1)
    source, panel_at, keep = pick(index), pick(block_row), pick(again)

    lanes = -(-local_blocks // LANES) * LANES
    place = (me % half_count) * per_owner + order
    cell = (group[None, :] == jnp.arange(2 * half_count, dtype=jnp.int32)[:, None])[:, None, :] & (
        block_offset[None, :] == jnp.arange(lanes, dtype=jnp.int32)[:, None]
    )[None]
    table = jnp.max(jnp.where(cell, place[None, None, :], -1), axis=2)
    table = jnp.where(table < 0, half_slots, table)
    table = table.reshape(2, half_count, 1, lanes).transpose(1, 0, 2, 3)
    table = jnp.broadcast_to(table, (half_count, 2, TILE, lanes)).reshape(half_count, 2 * TILE, lanes)

    panel_blocks = panel_rows.reshape(local_blocks, size, width)
    total = route(source, panel_at, keep, sparse_blocks, panel_blocks, table, row_half, per_owner)
    return total.reshape(local_blocks * size, width)


def solution(mesh):
    placed = (
        P(AXES, None, None),
        P(AXES, None),
        P(AXES),
        P(AXES, None),
        P(AXES),
    )
    return jax.shard_map(
        body, mesh=mesh, in_specs=placed, out_specs=P(AXES, None), check_vma=False
    )
```

```python
import functools

import jax
import jax.numpy as jnp
from jax import lax
from jax.experimental import pallas as pl
from jax.experimental.pallas import tpu as pltpu
from jax.sharding import PartitionSpec as P

AXES = ("row", "col")
VMEM_LIMIT = 67_000_000
LANES = 128
TILE = 8
SPILL = 1 << 20
MESH = pl.DeviceIdType.MESH


def split_parts(value):
    high = value.astype(jnp.bfloat16)
    low = (value - high.astype(jnp.float32)).astype(jnp.bfloat16)
    return high, low


def block_product(block, panel):
    block_high, block_low = split_parts(block)
    panel_high, panel_low = split_parts(panel)
    dims = (((0,), (0,)), ((), ()))
    dot = functools.partial(lax.dot_general, dimension_numbers=dims, preferred_element_type=jnp.float32)
    return dot(
        jnp.concatenate([block_high, block_low], axis=0),
        jnp.concatenate([panel_high, panel_high], axis=0),
    ) + dot(block_high, panel_low)


def peers_of(upper, lower, outer):
    moves = [
        (a, b, c) for a in range(upper) for b in range(lower) for c in range(outer) if (a, b, c) != (0, 0, 0)
    ]
    single = [move for move in moves if sum(digit > 0 for digit in move) == 1]
    double = [move for move in moves if sum(digit > 0 for digit in move) == 2]
    zeros = lambda move: tuple(digit == 0 for digit in move)
    order = sorted(single, key=zeros)
    opposite = sorted(double, key=lambda move: tuple(digit > 0 for digit in move))
    pairs = list(zip(order, opposite))
    first = [one for one, _ in pairs] + [other for _, other in pairs]
    second = [other for _, other in pairs] + [one for one, _ in pairs]
    rest = [move for move in moves if move not in first]
    return first + rest, second + rest


def route_kernel(
    row_half,
    per_owner,
    source_ref,
    panel_at_ref,
    keep_ref,
    sparse_hbm,
    panel_hbm,
    table_hbm,
    out_hbm,
    sparse,
    panel,
    products,
    far_land,
    near_land,
    sums,
    crossed,
    total,
    tables,
    near_table,
    far_table,
    data_send,
    data_recv,
    table_send,
    table_recv,
    cross_send,
    cross_recv,
    load_sems,
    own_sems,
    out_sems,
):
    row, col = lax.axis_index("row"), lax.axis_index("col")
    row_count, col_count = lax.axis_size("row"), lax.axis_size("col")
    half, inner = row // row_half, row % row_half
    outer, core = col // 2, col % 2
    lower = min(2, row_half)
    mine = inner * col_count + col
    count = row_half * col_count
    half_slots = count * per_owner
    upper_count, outer_count = row_half // lower, col_count // 2
    local_blocks = total.shape[0]
    chunk = min(8, local_blocks)
    chunks = local_blocks // chunk

    loads = [
        pltpu.make_async_copy(sparse_hbm, sparse, load_sems.at[0]),
        pltpu.make_async_copy(panel_hbm, panel, load_sems.at[1]),
    ]
    for load in loads:
        load.start()
    blank = jnp.zeros(far_land.shape[1:], jnp.float32)
    far_land[half_slots] = blank
    near_land[half_slots] = blank

    def target(move_pair, flip):
        one, other = move_pair
        a, b, c = (x + core * (y - x) for x, y in zip(one, other))
        there = (inner // lower + a) % upper_count * lower + (inner % lower + b) % lower
        beside = (outer + c) % outer_count * 2 + (core + flip) % 2
        number = ((a * lower + b) * outer_count + c) * 2 + flip
        return (half * row_half + there, beside), there * col_count + beside, number

    firsts, seconds = peers_of(upper_count, lower, outer_count)
    moves = list(zip(firsts, seconds))
    still = ((0, 0, 0), (0, 0, 0))
    targets = [target(move, (core + phase) % 2) for phase in range(2) for move in moves]
    targets.append(target(still, 1))
    opposite = ((row + row_half) % row_count, col)

    barrier = pltpu.get_barrier_semaphore()
    for device, _, _ in targets:
        pl.semaphore_signal(barrier, inc=1, device_id=device, device_id_type=MESH)
    pl.semaphore_signal(barrier, inc=1, device_id=opposite, device_id_type=MESH)
    pl.semaphore_wait(barrier, len(targets) + 1)

    def remote(source, destination, send_sem, recv_sem, device):
        copy = pltpu.make_async_remote_copy(
            src_ref=source,
            dst_ref=destination,
            send_sem=send_sem,
            recv_sem=recv_sem,
            device_id=device,
            device_id_type=MESH,
        )
        copy.start()
        return copy

    table_copies = [
        remote(table_hbm.at[place], tables.at[mine], table_send.at[number], table_recv.at[number], device)
        for device, place, number in targets
    ]
    own_table = pltpu.make_async_copy(table_hbm.at[mine], tables.at[mine], own_sems.at[0])
    own_table.start()
    for load in loads:
        load.wait()

    unit = min(4, per_owner)

    def fill(base, place, destination, at):
        first = base + place * per_owner

        def some(step, _):
            for k in range(unit):
                slot = step * unit + k
                source = source_ref[first + slot]
                product = block_product(sparse[source], panel[panel_at_ref[first + slot]])
                before = destination[at + jnp.maximum(slot - 1, 0)]
                product = product + jnp.where(keep_ref[first + slot] > 0, before, 0.0)
                destination[at + slot] = product
            return 0

        lax.fori_loop(0, per_owner // unit, some, 0)

    def spread(base, land, shift):
        copies = []
        for device, place, number in targets:
            at = base + place * per_owner
            fill(base, place, products, at)
            copies.append(
                remote(
                    products.at[pl.ds(at, per_owner)],
                    land.at[pl.ds(mine * per_owner, per_owner)],
                    data_send.at[shift + number],
                    data_recv.at[shift + number],
                    device,
                )
            )
        fill(base, mine, land, mine * per_owner)
        return copies

    far_copies = spread(half_slots, far_land, count)
    near_copies = spread(0, near_land, 0)

    own_table.wait()
    for copy in table_copies:
        copy.wait_recv()
    lookups = [
        pltpu.make_async_copy(tables.at[:, 0, :], near_table, own_sems.at[1]),
        pltpu.make_async_copy(tables.at[:, TILE, :], far_table, own_sems.at[2]),
    ]
    for lookup in lookups:
        lookup.start()
    for lookup in lookups:
        lookup.wait()

    def reduce(land, table, destination, first, number):
        def one(step, _):
            column = first + step
            value = land[table[0, column]]
            for origin in range(1, count):
                value = value + land[table[origin, column]]
            destination[column] = value
            return 0

        lax.fori_loop(0, number, one, 0)

    for copy in far_copies:
        copy.wait_recv()
    cross_copies = []
    for index in range(chunks):
        reduce(far_land, far_table, sums, index * chunk, chunk)
        part = pl.ds(index * chunk, chunk)
        cross_copies.append(
            remote(sums.at[part], crossed.at[part], cross_send.at[index], cross_recv.at[index], opposite)
        )
    for copy in near_copies:
        copy.wait_recv()
    reduce(near_land, near_table, total, 0, local_blocks)
    outs = []
    for index, copy in enumerate(cross_copies):
        copy.wait_recv()
        part = pl.ds(index * chunk, chunk)
        total[part] = total[part] + crossed[part]
        out = pltpu.make_async_copy(total.at[part], out_hbm.at[part], out_sems.at[index])
        out.start()
        outs.append(out)
    for copy in table_copies + far_copies + near_copies + cross_copies:
        copy.wait_send()
    for out in outs:
        out.wait()


def route(source, panel_at, keep, sparse_blocks, panel_blocks, table, row_half, per_owner):
    count = row_half * lax.axis_size("col")
    local_blocks, size, width = panel_blocks.shape
    half_slots = count * per_owner
    chunks = local_blocks // min(8, local_blocks)
    lanes = table.shape[-1]
    scalars = pl.BlockSpec(memory_space=pltpu.SMEM)
    anywhere = pl.BlockSpec(memory_space=pl.ANY)
    block = (size, width)
    dma = pltpu.SemaphoreType.DMA
    return pl.pallas_call(
        functools.partial(route_kernel, row_half, per_owner),
        in_specs=[scalars] * 3 + [anywhere] * 3,
        out_specs=anywhere,
        out_shape=jax.ShapeDtypeStruct((local_blocks,) + block, jnp.float32),
        scratch_shapes=[
            pltpu.VMEM(sparse_blocks.shape, jnp.float32),
            pltpu.VMEM(panel_blocks.shape, jnp.float32),
            pltpu.VMEM((2 * half_slots,) + block, jnp.float32),
            pltpu.VMEM((half_slots + 1,) + block, jnp.float32),
            pltpu.VMEM((half_slots + 1,) + block, jnp.float32),
            pltpu.VMEM((local_blocks,) + block, jnp.float32),
            pltpu.VMEM((local_blocks,) + block, jnp.float32),
            pltpu.VMEM((local_blocks,) + block, jnp.float32),
            pltpu.VMEM((count, 2 * TILE, lanes), jnp.int32),
            pltpu.SMEM((count, lanes), jnp.int32),
            pltpu.SMEM((count, lanes), jnp.int32),
            dma((2 * count,)),
            dma((2 * count,)),
            dma((count,)),
            dma((count,)),
            dma((chunks,)),
            dma((chunks,)),
            dma((2,)),
            dma((3,)),
            dma((chunks,)),
        ],
        compiler_params=pltpu.CompilerParams(
            collective_id=0, has_side_effects=True, vmem_limit_bytes=VMEM_LIMIT
        ),
    )(source, panel_at, keep, sparse_blocks, panel_blocks, table)


def layer_kernel(
    row_half,
    per_owner,
    first_list,
    slot_ref,
    sparse_hbm,
    panel_hbm,
    table_hbm,
    out_hbm,
    flag_ref,
    sparse,
    panel,
    products,
    far_land,
    near_land,
    list_one,
    list_two,
    sums,
    crossed,
    total,
    tables,
    spill,
    spill_in,
    near_table,
    far_table,
    starts,
    far_send,
    far_recv,
    near_send,
    near_recv,
    pass_send,
    pass_recv,
    list_send,
    list_recv,
    table_send,
    table_recv,
    cross_send,
    cross_recv,
    spill_sems,
    load_sems,
    own_sems,
    out_sems,
):
    row, col = lax.axis_index("row"), lax.axis_index("col")
    row_count, col_count = lax.axis_size("row"), lax.axis_size("col")
    half, inner = row // row_half, row % row_half
    outer, core = col // 2, col % 2
    lower = min(2, row_half)
    layer, beside_x = inner // lower, inner % lower
    mine = inner * col_count + col
    count = row_half * col_count
    around = lower * col_count
    half_slots = count * per_owner
    outer_count = col_count // 2
    rows_of_panel = panel.shape[0]
    local_blocks = total.shape[0]
    chunk = min(8, local_blocks)
    chunks = local_blocks // chunk
    second_list = list_two.shape[0]
    near_base, far_base, list_base = 0, around * per_owner, around * per_owner + half_slots

    loads = [
        pltpu.make_async_copy(sparse_hbm, sparse, load_sems.at[0]),
        pltpu.make_async_copy(panel_hbm, panel, load_sems.at[1]),
    ]
    for load in loads:
        load.start()
    blank = jnp.zeros(far_land.shape[1:], jnp.float32)
    far_land[half_slots] = blank
    near_land[half_slots] = blank

    def target(move_pair, flip):
        one, other = move_pair
        a, b, c = (x + core * (y - x) for x, y in zip(one, other))
        there = (layer + a) % 2 * lower + (beside_x + b) % lower
        beside = (outer + c) % outer_count * 2 + (core + flip) % 2
        number = ((a * lower + b) * outer_count + c) * 2 + flip
        return (half * row_half + there, beside), there * col_count + beside, number

    firsts, seconds = peers_of(2, lower, outer_count)
    moves = list(zip(firsts, seconds))
    flat = [move for move in firsts if move[0] == 0]
    flat_moves = list(zip(flat, sorted(flat, key=lambda move: (sum(move), move[1]))))
    still = ((0, 0, 0), (0, 0, 0))
    sibling = target(still, 1)
    partner_inner = (layer + 1) % 2 * lower + beside_x
    partner, partner_place = (half * row_half + partner_inner, col), partner_inner * col_count + col
    opposite = ((row + row_half) % row_count, col)

    everyone = [target(move, (core + phase) % 2) for phase in range(2) for move in moves] + [sibling]
    barrier = pltpu.get_barrier_semaphore()
    for device, _, _ in everyone:
        pl.semaphore_signal(barrier, inc=1, device_id=device, device_id_type=MESH)
    pl.semaphore_signal(barrier, inc=1, device_id=opposite, device_id_type=MESH)
    pl.semaphore_wait(barrier, len(everyone) + 1)

    def remote(source, destination, send_sem, recv_sem, device):
        return pltpu.make_async_remote_copy(
            src_ref=source,
            dst_ref=destination,
            send_sem=send_sem,
            recv_sem=recv_sem,
            device_id=device,
            device_id_type=MESH,
        )

    def begin(copy):
        copy.start()
        return copy

    table_copies = [
        begin(remote(table_hbm.at[place], tables.at[mine], table_send.at[number], table_recv.at[number], device))
        for device, place, number in everyone
    ]
    own_table = pltpu.make_async_copy(table_hbm.at[mine], tables.at[mine], own_sems.at[0])
    own_table.start()
    for load in loads:
        load.wait()

    def fill(base, slots, destination, at, lead=0):
        unit = min(4, slots)

        def some(step, _):
            for k in range(unit):
                slot = step * unit + k
                packed = slot_ref[base + slot]
                source, panel_at = packed // (2 * rows_of_panel), packed // 2 % rows_of_panel
                product = block_product(sparse[source], panel[panel_at])
                before = destination[at + jnp.maximum(slot - 1, -lead)]
                destination[at + slot] = product + jnp.where(packed % 2 > 0, before, 0.0)
            return 0

        lax.fori_loop(0, slots // unit, some, 0)

    def direct(base, index, land, send, recv, number, device):
        at = base + index * per_owner
        fill(at, per_owner, products, at)
        return begin(
            remote(
                products.at[pl.ds(at, per_owner)],
                land.at[pl.ds(mine * per_owner, per_owner)],
                send.at[number],
                recv.at[number],
                device,
            )
        )

    def send_far(device, place, number):
        return direct(far_base, place, far_land, far_send, far_recv, number, device)

    def send_near(device, place, number):
        return direct(near_base, place % around, near_land, near_send, near_recv, number, device)

    def send_list(first, land, index):
        slots = land.shape[0]
        fill(list_base + first, slots, products, list_base + first, min(first, 1))
        return remote(
            products.at[pl.ds(list_base + first, slots)], land, list_send.at[index], list_recv.at[index], partner
        )

    far_copies = [send_far(*target(move, core)) for move in moves]
    list_one_copy = begin(send_list(0, list_one, 0))
    far_copies += [send_far(*target(move, (core + 1) % 2)) for move in flat_moves]
    far_copies.append(send_far(*sibling))
    fill(far_base + mine * per_owner, per_owner, far_land, mine * per_owner)
    list_two_copy = send_list(first_list, list_two, 1)

    @pl.when(core == 1)
    def _():
        list_two_copy.start()

    near_targets = [target(move, (core + phase) % 2) for phase in range(2) for move in flat_moves] + [sibling]
    near_copies = [send_near(*one) for one in near_targets]
    fill(near_base + mine % around * per_owner, per_owner, near_land, mine * per_owner)

    own_table.wait()
    for copy in table_copies:
        copy.wait_recv()
    lookups = [
        pltpu.make_async_copy(tables.at[:, 0, :], near_table, own_sems.at[1]),
        pltpu.make_async_copy(tables.at[:, 1, :], far_table, own_sems.at[2]),
        pltpu.make_async_copy(tables.at[:, 2, :], starts, own_sems.at[3]),
    ]
    for lookup in lookups:
        lookup.start()
    worst = tables[0]
    for origin in range(1, count):
        worst = jnp.maximum(worst, tables[origin])
    spill[...] = worst
    spill_copy = begin(remote(spill, spill_in, spill_sems.at[0], spill_sems.at[1], opposite))
    for lookup in lookups:
        lookup.wait()

    def reduce(land, table, destination, first, number):
        def one(step, _):
            column = first + step
            value = land[table[0, column]]
            for origin in range(1, count):
                value = value + land[table[origin, column]]
            destination[column] = value
            return 0

        lax.fori_loop(0, number, one, 0)

    cross_copies = [
        remote(
            sums.at[pl.ds(index * chunk, chunk)],
            crossed.at[pl.ds(index * chunk, chunk)],
            cross_send.at[index],
            cross_recv.at[index],
            opposite,
        )
        for index in range(chunks)
    ]

    def cross():
        for index in range(chunks):
            reduce(far_land, far_table, sums, index * chunk, chunk)
            cross_copies[index].start()

    straight = [target(move, (core + phase) % 2) for phase in range(2) for move in flat_moves] + [sibling]
    level = lambda number, recv: remote(
        products.at[pl.ds(0, per_owner)],
        far_land.at[pl.ds(mine * per_owner, per_owner)],
        far_send.at[0],
        recv.at[number],
        partner,
    )

    def await_level():
        for _, _, number in straight:
            level(number, far_recv).wait_recv()

    @pl.when(core == 0)
    def _():
        await_level()
        for number in range(around, count):
            level(number, far_recv).wait_recv()
        cross()
        list_two_copy.start()

    relayed = []

    def relay(index, starting, land, shift, both):
        def pull(place, destination, at):
            start = starts[partner_place, starting(place % around)]

            def one(k, _):
                where = start + k
                value = list_one[jnp.minimum(where, first_list - 1)]
                if both:
                    other = list_two[jnp.clip(where - first_list, 0, second_list - 1)]
                    value = jnp.where(where < first_list, value, other)
                destination[at + k] = value
                return 0

            lax.fori_loop(0, per_owner, one, 0)

        def push(device, place, number):
            at = shift + place % around * per_owner
            pull(place, sparse, at)
            return begin(
                remote(
                    sparse.at[pl.ds(at, per_owner)],
                    land.at[pl.ds(partner_place * per_owner, per_owner)],
                    pass_send.at[index * around + number],
                    pass_recv.at[index * around + number],
                    device,
                )
            )

        def keep():
            pull(mine, land, partner_place * per_owner)

        return push, keep

    push_far, keep_far = relay(0, lambda place: place // 2, far_land, 0, False)
    push_near, keep_near = relay(
        1, lambda place: around // 2 + place, near_land, around * per_owner, True
    )
    sibling_pass = lambda index, land: remote(
        sparse.at[pl.ds(0, per_owner)],
        land.at[pl.ds(partner_place * per_owner, per_owner)],
        pass_send.at[index * around + 1],
        pass_recv.at[index * around + 1],
        sibling[0],
    )

    list_one_copy.wait_recv()
    far_passes = [push_far(*target(move, (core + 1) % 2)) for move in flat_moves]

    @pl.when(core == 0)
    def _():
        push_far(*sibling)

    @pl.when(core == 1)
    def _():
        keep_far()
        await_level()
        for _, _, number in straight:
            level(number, pass_recv).wait_recv()
        cross()

    list_two_copy.wait_recv()
    near_passes = [push_near(*one) for one in near_targets]
    keep_near()

    spill_copy.wait_recv()
    flag_ref[...] = jnp.maximum(spill[...], spill_in[...])
    for copy in near_copies + near_passes:
        copy.wait_recv()
    reduce(near_land, near_table, total, 0, local_blocks)
    outs = []
    for index, copy in enumerate(cross_copies):
        copy.wait_recv()
        part = pl.ds(index * chunk, chunk)
        total[part] = total[part] + crossed[part]
        out = pltpu.make_async_copy(total.at[part], out_hbm.at[part], out_sems.at[index])
        out.start()
        outs.append(out)
    sent = table_copies + far_copies + [list_one_copy, list_two_copy] + near_copies
    for copy in sent + far_passes + near_passes + cross_copies + [spill_copy]:
        copy.wait_send()

    @pl.when(core == 0)
    def _():
        sibling_pass(0, far_land).wait_send()

    for out in outs:
        out.wait()


def route_layers(slots, sparse_blocks, panel_blocks, table, row_half, per_owner, first_list, list_slots):
    count = row_half * lax.axis_size("col")
    around = count // 2
    local_blocks, size, width = panel_blocks.shape
    half_slots = count * per_owner
    chunks = local_blocks // min(8, local_blocks)
    lanes = table.shape[-1]
    scalars = pl.BlockSpec(memory_space=pltpu.SMEM)
    anywhere = pl.BlockSpec(memory_space=pl.ANY)
    block = (size, width)
    dma = pltpu.SemaphoreType.DMA
    blocks = lambda number: pltpu.VMEM((number,) + block, jnp.float32)
    return pl.pallas_call(
        functools.partial(layer_kernel, row_half, per_owner, first_list),
        in_specs=[scalars] + [anywhere] * 3,
        out_specs=[anywhere, pl.BlockSpec(memory_space=pltpu.VMEM)],
        out_shape=[
            jax.ShapeDtypeStruct((local_blocks,) + block, jnp.float32),
            jax.ShapeDtypeStruct((TILE, lanes), jnp.int32),
        ],
        scratch_shapes=[
            pltpu.VMEM(sparse_blocks.shape, jnp.float32),
            pltpu.VMEM(panel_blocks.shape, jnp.float32),
            blocks(around * per_owner + half_slots + list_slots),
            blocks(half_slots + 1),
            blocks(half_slots + 1),
            blocks(first_list),
            blocks(list_slots - first_list),
            blocks(local_blocks),
            blocks(local_blocks),
            blocks(local_blocks),
            pltpu.VMEM((count, TILE, lanes), jnp.int32),
            pltpu.VMEM((TILE, lanes), jnp.int32),
            pltpu.VMEM((TILE, lanes), jnp.int32),
            pltpu.SMEM((count, lanes), jnp.int32),
            pltpu.SMEM((count, lanes), jnp.int32),
            pltpu.SMEM((count, lanes), jnp.int32),
            dma((count,)),
            dma((count,)),
            dma((around,)),
            dma((around,)),
            dma((2 * around,)),
            dma((2 * around,)),
            dma((2,)),
            dma((2,)),
            dma((count,)),
            dma((count,)),
            dma((chunks,)),
            dma((chunks,)),
            dma((2,)),
            dma((2,)),
            dma((4,)),
            dma((chunks,)),
        ],
        compiler_params=pltpu.CompilerParams(
            collective_id=1, has_side_effects=True, vmem_limit_bytes=VMEM_LIMIT
        ),
    )(slots, sparse_blocks, panel_blocks, table)


def body(sparse_blocks, panel_rows, block_row, block_owner, block_offset):
    device_count = lax.axis_size("row") * lax.axis_size("col")
    half_count = device_count // 2
    slot_count, size, _ = sparse_blocks.shape
    width = panel_rows.shape[1]
    local_blocks = panel_rows.shape[0] // size
    per_owner = max(2, 2 * slot_count // device_count)
    half_slots = half_count * per_owner
    me = lax.axis_index(AXES)
    my_half = me // half_count
    row_half = lax.axis_size("row") // 2
    owner = block_owner[:, 0]
    index = jnp.arange(slot_count, dtype=jnp.int32)
    key = block_offset * slot_count + index
    same = owner[:, None] == owner[None, :]
    earlier = same & (key[None, :] < key[:, None])
    order = jnp.sum(earlier.astype(jnp.int32), axis=1)
    again = jnp.any(earlier & (block_offset[None, :] == block_offset[:, None]), axis=1).astype(jnp.int32)
    far = (owner // half_count != my_half).astype(jnp.int32)
    place = owner % half_count
    panel_blocks = panel_rows.reshape(local_blocks, size, width)
    lanes = -(-max(local_blocks, LANES) // LANES) * LANES

    landing = (me % half_count) * per_owner + order
    group = far * half_count + place
    cell = (group[None, :] == jnp.arange(2 * half_count, dtype=jnp.int32)[:, None])[:, None, :] & (
        block_offset[None, :] == jnp.arange(lanes, dtype=jnp.int32)[:, None]
    )[None]
    table = jnp.max(jnp.where(cell, landing[None, None, :], -1), axis=2)
    table = jnp.where(table < 0, half_slots, table).reshape(2, half_count, 1, lanes)

    def whole():
        position = group * per_owner + order
        hit = position[None, :] == jnp.arange(2 * half_slots, dtype=jnp.int32)[:, None]
        pick = lambda value: jnp.max(jnp.where(hit, value[None, :], 0), axis=1)
        pair = table.transpose(1, 0, 2, 3)
        pair = jnp.broadcast_to(pair, (half_count, 2, TILE, lanes)).reshape(half_count, 2 * TILE, lanes)
        return route(
            pick(index), pick(block_row), pick(again), sparse_blocks, panel_blocks, pair, row_half, per_owner
        )

    lower = min(2, row_half)
    around = lower * lax.axis_size("col")
    if half_count != 2 * around or local_blocks < 8:
        return whole().reshape(local_blocks * size, width)

    first_list = around // 2 * per_owner
    list_slots = max(slot_count // 2, first_list + 8)
    beyond = place // around != (me % half_count) // around
    flat_place = place % around
    listed = beyond & ((far == 0) | (flat_place % 2 == 1))
    list_group = jnp.where(far == 1, flat_place // 2, around // 2 + flat_place)
    list_group = jnp.where(listed, list_group, lanes)
    ahead = jnp.sum((list_group[None, :] < list_group[:, None]).astype(jnp.int32), axis=1)
    starts = jnp.sum(
        (list_group[None, :] < jnp.arange(lanes, dtype=jnp.int32)[:, None]).astype(jnp.int32), axis=1
    )
    spilled = jnp.sum(listed.astype(jnp.int32)) > list_slots
    starts = jnp.where(jnp.arange(lanes) == lanes - 1, jnp.where(spilled, SPILL, 0), starts)
    list_base = around * per_owner + half_slots
    position = jnp.where(
        listed,
        list_base + ahead + order,
        jnp.where(far == 1, around * per_owner + place * per_owner + order, flat_place * per_owner + order),
    )
    packed = (index * local_blocks + block_row) * 2 + again
    hit = position[None, :] == jnp.arange(list_base + list_slots, dtype=jnp.int32)[:, None]
    slots = jnp.max(jnp.where(hit, packed[None, :], 0), axis=1)
    kind = jnp.arange(TILE, dtype=jnp.int32)[None, :, None]
    rows = jnp.where(kind == 0, table[0], jnp.where(kind == 1, table[1], starts[None, None, :]))
    total, flags = route_layers(
        slots, sparse_blocks, panel_blocks, rows, row_half, per_owner, first_list, list_slots
    )
    total = lax.cond(flags[2, lanes - 1] >= SPILL, whole, lambda: total)
    return total.reshape(local_blocks * size, width)


def solution(mesh):
    placed = (
        P(AXES, None, None),
        P(AXES, None),
        P(AXES),
        P(AXES, None),
        P(AXES),
    )
    return jax.shard_map(
        body, mesh=mesh, in_specs=placed, out_specs=P(AXES, None), check_vma=False
    )
```

```python
import functools

import jax
import jax.numpy as jnp
from jax import lax
from jax.experimental import pallas as pl
from jax.experimental.pallas import tpu as pltpu
from jax.sharding import PartitionSpec as P

AXES = ("row", "col")
VMEM_LIMIT = 67_000_000
LANES = 128
TILE = 8
SPILL = 1 << 20
MESH = pl.DeviceIdType.MESH


def split_parts(value):
    high = value.astype(jnp.bfloat16)
    low = (value - high.astype(jnp.float32)).astype(jnp.bfloat16)
    return high, low


def block_product(block, panel):
    block_high, block_low = split_parts(block)
    panel_high, panel_low = split_parts(panel)
    dims = (((0,), (0,)), ((), ()))
    dot = functools.partial(lax.dot_general, dimension_numbers=dims, preferred_element_type=jnp.float32)
    return dot(
        jnp.concatenate([block_high, block_low], axis=0),
        jnp.concatenate([panel_high, panel_high], axis=0),
    ) + dot(block_high, panel_low)


def peers_of(upper, lower, outer):
    moves = [
        (a, b, c) for a in range(upper) for b in range(lower) for c in range(outer) if (a, b, c) != (0, 0, 0)
    ]
    single = [move for move in moves if sum(digit > 0 for digit in move) == 1]
    double = [move for move in moves if sum(digit > 0 for digit in move) == 2]
    zeros = lambda move: tuple(digit == 0 for digit in move)
    order = sorted(single, key=zeros)
    opposite = sorted(double, key=lambda move: tuple(digit > 0 for digit in move))
    pairs = list(zip(order, opposite))
    first = [one for one, _ in pairs] + [other for _, other in pairs]
    second = [other for _, other in pairs] + [one for one, _ in pairs]
    rest = [move for move in moves if move not in first]
    return first + rest, second + rest


def route_kernel(
    row_half,
    per_owner,
    source_ref,
    panel_at_ref,
    keep_ref,
    sparse_hbm,
    panel_hbm,
    table_hbm,
    out_hbm,
    sparse,
    panel,
    products,
    far_land,
    near_land,
    sums,
    crossed,
    total,
    tables,
    near_table,
    far_table,
    data_send,
    data_recv,
    table_send,
    table_recv,
    cross_send,
    cross_recv,
    load_sems,
    own_sems,
    out_sems,
):
    row, col = lax.axis_index("row"), lax.axis_index("col")
    row_count, col_count = lax.axis_size("row"), lax.axis_size("col")
    half, inner = row // row_half, row % row_half
    outer, core = col // 2, col % 2
    lower = min(2, row_half)
    mine = inner * col_count + col
    count = row_half * col_count
    half_slots = count * per_owner
    upper_count, outer_count = row_half // lower, col_count // 2
    local_blocks = total.shape[0]
    chunk = min(8, local_blocks)
    chunks = local_blocks // chunk

    loads = [
        pltpu.make_async_copy(sparse_hbm, sparse, load_sems.at[0]),
        pltpu.make_async_copy(panel_hbm, panel, load_sems.at[1]),
    ]
    for load in loads:
        load.start()
    blank = jnp.zeros(far_land.shape[1:], jnp.float32)
    far_land[half_slots] = blank
    near_land[half_slots] = blank

    def target(move_pair, flip):
        one, other = move_pair
        a, b, c = (x + core * (y - x) for x, y in zip(one, other))
        there = (inner // lower + a) % upper_count * lower + (inner % lower + b) % lower
        beside = (outer + c) % outer_count * 2 + (core + flip) % 2
        number = ((a * lower + b) * outer_count + c) * 2 + flip
        return (half * row_half + there, beside), there * col_count + beside, number

    firsts, seconds = peers_of(upper_count, lower, outer_count)
    moves = list(zip(firsts, seconds))
    still = ((0, 0, 0), (0, 0, 0))
    targets = [target(move, (core + phase) % 2) for phase in range(2) for move in moves]
    targets.append(target(still, 1))
    opposite = ((row + row_half) % row_count, col)

    barrier = pltpu.get_barrier_semaphore()
    for device, _, _ in targets:
        pl.semaphore_signal(barrier, inc=1, device_id=device, device_id_type=MESH)
    pl.semaphore_signal(barrier, inc=1, device_id=opposite, device_id_type=MESH)
    pl.semaphore_wait(barrier, len(targets) + 1)

    def remote(source, destination, send_sem, recv_sem, device):
        copy = pltpu.make_async_remote_copy(
            src_ref=source,
            dst_ref=destination,
            send_sem=send_sem,
            recv_sem=recv_sem,
            device_id=device,
            device_id_type=MESH,
        )
        copy.start()
        return copy

    table_copies = [
        remote(table_hbm.at[place], tables.at[mine], table_send.at[number], table_recv.at[number], device)
        for device, place, number in targets
    ]
    own_table = pltpu.make_async_copy(table_hbm.at[mine], tables.at[mine], own_sems.at[0])
    own_table.start()
    for load in loads:
        load.wait()

    unit = min(4, per_owner)

    def fill(base, place, destination, at):
        first = base + place * per_owner

        def some(step, _):
            for k in range(unit):
                slot = step * unit + k
                source = source_ref[first + slot]
                product = block_product(sparse[source], panel[panel_at_ref[first + slot]])
                before = destination[at + jnp.maximum(slot - 1, 0)]
                product = product + jnp.where(keep_ref[first + slot] > 0, before, 0.0)
                destination[at + slot] = product
            return 0

        lax.fori_loop(0, per_owner // unit, some, 0)

    def spread(base, land, shift):
        copies = []
        for device, place, number in targets:
            at = base + place * per_owner
            fill(base, place, products, at)
            copies.append(
                remote(
                    products.at[pl.ds(at, per_owner)],
                    land.at[pl.ds(mine * per_owner, per_owner)],
                    data_send.at[shift + number],
                    data_recv.at[shift + number],
                    device,
                )
            )
        fill(base, mine, land, mine * per_owner)
        return copies

    far_copies = spread(half_slots, far_land, count)
    near_copies = spread(0, near_land, 0)

    own_table.wait()
    for copy in table_copies:
        copy.wait_recv()
    lookups = [
        pltpu.make_async_copy(tables.at[:, 0, :], near_table, own_sems.at[1]),
        pltpu.make_async_copy(tables.at[:, TILE, :], far_table, own_sems.at[2]),
    ]
    for lookup in lookups:
        lookup.start()
    for lookup in lookups:
        lookup.wait()

    def reduce(land, table, destination, first, number):
        def one(step, _):
            column = first + step
            value = land[table[0, column]]
            for origin in range(1, count):
                value = value + land[table[origin, column]]
            destination[column] = value
            return 0

        lax.fori_loop(0, number, one, 0)

    for copy in far_copies:
        copy.wait_recv()
    cross_copies = []
    for index in range(chunks):
        reduce(far_land, far_table, sums, index * chunk, chunk)
        part = pl.ds(index * chunk, chunk)
        cross_copies.append(
            remote(sums.at[part], crossed.at[part], cross_send.at[index], cross_recv.at[index], opposite)
        )
    for copy in near_copies:
        copy.wait_recv()
    reduce(near_land, near_table, total, 0, local_blocks)
    outs = []
    for index, copy in enumerate(cross_copies):
        copy.wait_recv()
        part = pl.ds(index * chunk, chunk)
        total[part] = total[part] + crossed[part]
        out = pltpu.make_async_copy(total.at[part], out_hbm.at[part], out_sems.at[index])
        out.start()
        outs.append(out)
    for copy in table_copies + far_copies + near_copies + cross_copies:
        copy.wait_send()
    for out in outs:
        out.wait()


def route(source, panel_at, keep, sparse_blocks, panel_blocks, table, row_half, per_owner):
    count = row_half * lax.axis_size("col")
    local_blocks, size, width = panel_blocks.shape
    half_slots = count * per_owner
    chunks = local_blocks // min(8, local_blocks)
    lanes = table.shape[-1]
    scalars = pl.BlockSpec(memory_space=pltpu.SMEM)
    anywhere = pl.BlockSpec(memory_space=pl.ANY)
    block = (size, width)
    dma = pltpu.SemaphoreType.DMA
    return pl.pallas_call(
        functools.partial(route_kernel, row_half, per_owner),
        in_specs=[scalars] * 3 + [anywhere] * 3,
        out_specs=anywhere,
        out_shape=jax.ShapeDtypeStruct((local_blocks,) + block, jnp.float32),
        scratch_shapes=[
            pltpu.VMEM(sparse_blocks.shape, jnp.float32),
            pltpu.VMEM(panel_blocks.shape, jnp.float32),
            pltpu.VMEM((2 * half_slots,) + block, jnp.float32),
            pltpu.VMEM((half_slots + 1,) + block, jnp.float32),
            pltpu.VMEM((half_slots + 1,) + block, jnp.float32),
            pltpu.VMEM((local_blocks,) + block, jnp.float32),
            pltpu.VMEM((local_blocks,) + block, jnp.float32),
            pltpu.VMEM((local_blocks,) + block, jnp.float32),
            pltpu.VMEM((count, 2 * TILE, lanes), jnp.int32),
            pltpu.SMEM((count, lanes), jnp.int32),
            pltpu.SMEM((count, lanes), jnp.int32),
            dma((2 * count,)),
            dma((2 * count,)),
            dma((count,)),
            dma((count,)),
            dma((chunks,)),
            dma((chunks,)),
            dma((2,)),
            dma((3,)),
            dma((chunks,)),
        ],
        compiler_params=pltpu.CompilerParams(
            collective_id=0, has_side_effects=True, vmem_limit_bytes=VMEM_LIMIT
        ),
    )(source, panel_at, keep, sparse_blocks, panel_blocks, table)


def layer_kernel(
    row_half,
    per_owner,
    first_list,
    slot_ref,
    sparse_hbm,
    panel_hbm,
    table_hbm,
    out_hbm,
    flag_ref,
    sparse,
    panel,
    products,
    far_land,
    near_land,
    list_one,
    list_two,
    sums,
    crossed,
    total,
    tables,
    spill,
    spill_in,
    near_table,
    far_table,
    starts,
    far_send,
    far_recv,
    near_send,
    near_recv,
    pass_send,
    pass_recv,
    list_send,
    list_recv,
    table_send,
    table_recv,
    cross_send,
    cross_recv,
    spill_sems,
    load_sems,
    own_sems,
    out_sems,
    beside_sems,
    across_sems,
):
    row, col = lax.axis_index("row"), lax.axis_index("col")
    col_count = lax.axis_size("col")
    half, inner = row // row_half, row % row_half
    outer, core = col // 2, col % 2
    lower = min(2, row_half)
    layer, beside_x = inner // lower, inner % lower
    mine = inner * col_count + col
    count = row_half * col_count
    around = lower * col_count
    half_slots = count * per_owner
    outer_count = col_count // 2
    rows_of_panel = panel.shape[0]
    local_blocks = total.shape[0]
    chunk = min(8, local_blocks)
    chunks = local_blocks // chunk
    second_list = list_two.shape[0]
    near_base, far_base, list_base = 0, around * per_owner, around * per_owner + half_slots

    loads = [
        pltpu.make_async_copy(sparse_hbm, sparse, load_sems.at[0]),
        pltpu.make_async_copy(panel_hbm, panel, load_sems.at[1]),
    ]
    for load in loads:
        load.start()
    blank = jnp.zeros(far_land.shape[1:], jnp.float32)
    far_land[half_slots] = blank
    near_land[half_slots] = blank

    def target(move_pair, flip):
        one, other = move_pair
        a, b, c = (x + core * (y - x) for x, y in zip(one, other))
        there = (layer + a) % 2 * lower + (beside_x + b) % lower
        beside = (outer + c) % outer_count * 2 + (core + flip) % 2
        number = ((a * lower + b) * outer_count + c) * 2 + flip
        return (half * row_half + there, beside), there * col_count + beside, number

    firsts, seconds = peers_of(2, lower, outer_count)
    moves = list(zip(firsts, seconds))
    flat = [move for move in firsts if move[0] == 0]
    flat_moves = list(zip(flat, sorted(flat, key=lambda move: (sum(move), move[1]))))
    still = ((0, 0, 0), (0, 0, 0))
    sibling = target(still, 1)
    partner_inner = (layer + 1) % 2 * lower + beside_x
    partner, partner_place = (half * row_half + partner_inner, col), partner_inner * col_count + col
    opposite = ((1 - half) * row_half + (1 - layer) * lower + beside_x, col)

    everyone = [target(move, (core + phase) % 2) for phase in range(2) for move in moves] + [sibling]
    barrier = pltpu.get_barrier_semaphore()
    for device, _, _ in everyone:
        pl.semaphore_signal(barrier, inc=1, device_id=device, device_id_type=MESH)
    pl.semaphore_signal(barrier, inc=1, device_id=opposite, device_id_type=MESH)
    with jax.named_scope("barrier"):
        pl.semaphore_wait(barrier, len(everyone) + 1)

    def remote(source, destination, send_sem, recv_sem, device):
        return pltpu.make_async_remote_copy(
            src_ref=source,
            dst_ref=destination,
            send_sem=send_sem,
            recv_sem=recv_sem,
            device_id=device,
            device_id_type=MESH,
        )

    def begin(copy):
        copy.start()
        return copy

    table_copies = [
        begin(remote(table_hbm.at[place], tables.at[mine], table_send.at[number], table_recv.at[number], device))
        for device, place, number in everyone
    ]
    own_table = pltpu.make_async_copy(table_hbm.at[mine], tables.at[mine], own_sems.at[0])
    own_table.start()
    with jax.named_scope("load_wait"):
        for load in loads:
            load.wait()

    def fill(base, slots, destination, at, lead=0):
        unit = min(4, slots)

        def some(step, _):
            for k in range(unit):
                slot = step * unit + k
                packed = slot_ref[base + slot]
                source, panel_at = packed // (2 * rows_of_panel), packed // 2 % rows_of_panel
                product = block_product(sparse[source], panel[panel_at])
                before = destination[at + jnp.maximum(slot - 1, -lead)]
                destination[at + slot] = product + jnp.where(packed % 2 > 0, before, 0.0)
            return 0

        lax.fori_loop(0, slots // unit, some, 0)

    def direct(base, index, land, send, recv, number, device, later=False):
        at = base + index * per_owner
        copy = remote(
            products.at[pl.ds(at, per_owner)],
            land.at[pl.ds(mine * per_owner, per_owner)],
            send.at[number],
            recv.at[number],
            device,
        )

        fill(at, per_owner, products, at)
        if not later:
            copy.start()
        return copy

    def send_far(device, place, number):
        return direct(far_base, place, far_land, far_send, far_recv, number, device)

    def send_near(device, place, number):
        return direct(near_base, place % around, near_land, near_send, near_recv, number, device, True)

    def send_list(first, land, index):
        slots = land.shape[0]
        fill(list_base + first, slots, products, list_base + first, min(first, 1))
        return remote(
            products.at[pl.ds(list_base + first, slots)], land, list_send.at[index], list_recv.at[index], partner
        )

    with jax.named_scope("far_first"):
        far_copies = [send_far(*target(move, core)) for move in moves]
    with jax.named_scope("list_one"):
        list_one_copy = begin(send_list(0, list_one, 0))
    with jax.named_scope("far_second"):
        far_copies += [send_far(*target(move, (core + 1) % 2)) for move in flat_moves]
        far_copies.append(send_far(*sibling))
        fill(far_base + mine * per_owner, per_owner, far_land, mine * per_owner)
    with jax.named_scope("list_two"):
        list_two_copy = send_list(first_list, list_two, 1)

    at_end = layer == half

    near_targets = [target(move, (core + phase) % 2) for phase in range(2) for move in flat_moves] + [sibling]
    with jax.named_scope("near_own"):
        near_copies = [send_near(*one) for one in near_targets]
        fill(near_base + mine % around * per_owner, per_owner, near_land, mine * per_owner)

    def start_near():
        for copy in near_copies:
            copy.start()

    with jax.named_scope("table_wait"):
        own_table.wait()
        for copy in table_copies:
            copy.wait_recv()
    lookups = [
        pltpu.make_async_copy(tables.at[:, 0, :], near_table, own_sems.at[1]),
        pltpu.make_async_copy(tables.at[:, 1, :], far_table, own_sems.at[2]),
        pltpu.make_async_copy(tables.at[:, 2, :], starts, own_sems.at[3]),
    ]
    for lookup in lookups:
        lookup.start()
    worst = tables[0]
    for origin in range(1, count):
        worst = jnp.maximum(worst, tables[origin])
    spill[...] = worst
    spill_copy = begin(remote(spill, spill_in, spill_sems.at[0], spill_sems.at[1], opposite))
    for lookup in lookups:
        lookup.wait()

    def reduce(land, table, destination, first, number):
        def one(step, _):
            column = first + step
            value = land[table[0, column]]
            for origin in range(1, count):
                value = value + land[table[origin, column]]
            destination[column] = value
            return 0

        lax.fori_loop(0, number, one, 0)

    cross_copies = [
        remote(
            sums.at[pl.ds(index * chunk, chunk)],
            crossed.at[pl.ds(index * chunk, chunk)],
            cross_send.at[index],
            cross_recv.at[index],
            opposite,
        )
        for index in range(chunks)
    ]

    def cross(held=False):
        for index in range(chunks):
            reduce(far_land, far_table, sums, index * chunk, chunk)
            if not held:
                cross_copies[index].start()

    straight = [target(move, (core + phase) % 2) for phase in range(2) for move in flat_moves] + [sibling]
    level = lambda number, recv: remote(
        products.at[pl.ds(0, per_owner)],
        far_land.at[pl.ds(mine * per_owner, per_owner)],
        far_send.at[0],
        recv.at[number],
        partner,
    )

    def await_level():
        for _, _, number in straight:
            level(number, far_recv).wait_recv()

    @pl.when(core == 0)
    def _():
        with jax.named_scope("far_wait"):
            await_level()
            for number in range(around, count):
                level(number, far_recv).wait_recv()
        @pl.when(at_end)
        def _():
            with jax.named_scope("cross_early"):
                cross(True)

        @pl.when(jnp.logical_not(at_end))
        def _():
            with jax.named_scope("cross_early"):
                cross()

    def relay(index, starting, land, shift, both):
        def pull(place, destination, at):
            start = starts[partner_place, starting(place % around)]

            def one(k, _):
                where = start + k
                value = list_one[jnp.minimum(where, first_list - 1)]
                if both:
                    other = list_two[jnp.clip(where - first_list, 0, second_list - 1)]
                    value = jnp.where(where < first_list, value, other)
                destination[at + k] = value
                return 0

            lax.fori_loop(0, per_owner, one, 0)

        def push(device, place, number):
            at = shift + place % around * per_owner
            pull(place, sparse, at)
            return begin(
                remote(
                    sparse.at[pl.ds(at, per_owner)],
                    land.at[pl.ds(partner_place * per_owner, per_owner)],
                    pass_send.at[index * around + number],
                    pass_recv.at[index * around + number],
                    device,
                )
            )

        def keep():
            pull(mine, land, partner_place * per_owner)

        return push, keep

    push_far, keep_far = relay(0, lambda place: place // 2, far_land, 0, False)
    push_near, keep_near = relay(
        1, lambda place: around // 2 + place, near_land, around * per_owner, True
    )
    sibling_pass = lambda index, land: remote(
        sparse.at[pl.ds(0, per_owner)],
        land.at[pl.ds(partner_place * per_owner, per_owner)],
        pass_send.at[index * around + 1],
        pass_recv.at[index * around + 1],
        sibling[0],
    )

    with jax.named_scope("list_one_wait"):
        list_one_copy.wait_recv()

    @pl.when(jnp.logical_not(at_end))
    def _():
        list_two_copy.start()
    with jax.named_scope("pass_far"):
        far_passes = [push_far(*target(move, (core + 1) % 2)) for move in flat_moves]

    @pl.when(core == 0)
    def _():
        push_far(*sibling)

    @pl.when(at_end & (core == 1))
    def _():
        pl.semaphore_signal(beside_sems.at[0], inc=1, device_id=sibling[0], device_id_type=MESH)

    @pl.when(at_end & (core == 0))
    def _():
        pl.semaphore_wait(beside_sems.at[0], 1)
        pl.semaphore_signal(across_sems.at[0], inc=1, device_id=opposite, device_id_type=MESH)
        pl.semaphore_wait(across_sems.at[0], 1)
        for copy in cross_copies:
            copy.start()
        list_two_copy.start()

    start_near()

    @pl.when(core == 1)
    def _():
        keep_far()
        with jax.named_scope("pass_far_wait"):
            await_level()
            for _, _, number in straight:
                level(number, pass_recv).wait_recv()

        @pl.when(at_end)
        def _():
            list_two_copy.start()
            with jax.named_scope("cross_late"):
                cross(True)

        @pl.when(jnp.logical_not(at_end))
        def _():
            with jax.named_scope("cross_late"):
                cross()

    with jax.named_scope("list_two_wait"):
        list_two_copy.wait_recv()
    with jax.named_scope("pass_near"):
        near_passes = [push_near(*one) for one in near_targets]
        keep_near()

    @pl.when(at_end & (core == 0))
    def _():
        pl.semaphore_signal(beside_sems.at[1], inc=1, device_id=sibling[0], device_id_type=MESH)

    @pl.when(at_end & (core == 1))
    def _():
        pl.semaphore_wait(beside_sems.at[1], 1)
        pl.semaphore_signal(across_sems.at[1], inc=1, device_id=opposite, device_id_type=MESH)
        pl.semaphore_wait(across_sems.at[1], 1)
        for copy in cross_copies:
            copy.start()


    spill_copy.wait()
    spill[...] = jnp.maximum(spill[...], spill_in[...])
    flag_copy = pltpu.make_async_copy(spill.at[2], starts.at[0], own_sems.at[0])
    flag_copy.start()
    flag_copy.wait()
    flag_ref[0, 0] = starts[0, starts.shape[1] - 1]
    with jax.named_scope("near_wait"):
        for copy in near_copies + near_passes:
            copy.wait_recv()
    with jax.named_scope("near_sum"):
        reduce(near_land, near_table, total, 0, local_blocks)
    outs = []
    for index, copy in enumerate(cross_copies):
        with jax.named_scope(f"cross_wait{index}"):
            copy.wait_recv()
        part = pl.ds(index * chunk, chunk)
        total[part] = total[part] + crossed[part]
        out = pltpu.make_async_copy(total.at[part], out_hbm.at[part], out_sems.at[index])
        out.start()
        outs.append(out)
    sent = table_copies + far_copies + [list_one_copy, list_two_copy] + near_copies
    for copy in sent + far_passes + near_passes + cross_copies:
        copy.wait_send()

    @pl.when(core == 0)
    def _():
        sibling_pass(0, far_land).wait_send()

    for out in outs:
        out.wait()


def route_layers(slots, sparse_blocks, panel_blocks, table, row_half, per_owner, first_list, list_slots):
    count = row_half * lax.axis_size("col")
    around = count // 2
    local_blocks, size, width = panel_blocks.shape
    half_slots = count * per_owner
    chunks = local_blocks // min(8, local_blocks)
    lanes = table.shape[-1]
    scalars = pl.BlockSpec(memory_space=pltpu.SMEM)
    anywhere = pl.BlockSpec(memory_space=pl.ANY)
    block = (size, width)
    dma = pltpu.SemaphoreType.DMA
    blocks = lambda number: pltpu.VMEM((number,) + block, jnp.float32)
    return pl.pallas_call(
        functools.partial(layer_kernel, row_half, per_owner, first_list),
        in_specs=[scalars] + [anywhere] * 3,
        out_specs=[anywhere, scalars],
        out_shape=[
            jax.ShapeDtypeStruct((local_blocks,) + block, jnp.float32),
            jax.ShapeDtypeStruct((1, 1), jnp.int32),
        ],
        scratch_shapes=[
            pltpu.VMEM(sparse_blocks.shape, jnp.float32),
            pltpu.VMEM(panel_blocks.shape, jnp.float32),
            blocks(around * per_owner + half_slots + list_slots),
            blocks(half_slots + 1),
            blocks(half_slots + 1),
            blocks(first_list),
            blocks(list_slots - first_list),
            blocks(local_blocks),
            blocks(local_blocks),
            blocks(local_blocks),
            pltpu.VMEM((count, TILE, lanes), jnp.int32),
            pltpu.VMEM((TILE, lanes), jnp.int32),
            pltpu.VMEM((TILE, lanes), jnp.int32),
            pltpu.SMEM((count, lanes), jnp.int32),
            pltpu.SMEM((count, lanes), jnp.int32),
            pltpu.SMEM((count, lanes), jnp.int32),
            dma((count,)),
            dma((count,)),
            dma((around,)),
            dma((around,)),
            dma((2 * around,)),
            dma((2 * around,)),
            dma((2,)),
            dma((2,)),
            dma((count,)),
            dma((count,)),
            dma((chunks,)),
            dma((chunks,)),
            dma((2,)),
            dma((2,)),
            dma((4,)),
            dma((chunks,)),
            pltpu.SemaphoreType.REGULAR((2,)),
            pltpu.SemaphoreType.REGULAR((2,)),
        ],
        compiler_params=pltpu.CompilerParams(
            collective_id=1, has_side_effects=True, vmem_limit_bytes=VMEM_LIMIT
        ),
    )(slots, sparse_blocks, panel_blocks, table)


def body(sparse_blocks, panel_rows, block_row, block_owner, block_offset):
    device_count = lax.axis_size("row") * lax.axis_size("col")
    half_count = device_count // 2
    slot_count, size, _ = sparse_blocks.shape
    width = panel_rows.shape[1]
    local_blocks = panel_rows.shape[0] // size
    per_owner = max(2, 2 * slot_count // device_count)
    half_slots = half_count * per_owner
    me = lax.axis_index(AXES)
    my_half = me // half_count
    row_half = lax.axis_size("row") // 2
    owner = block_owner[:, 0]
    index = jnp.arange(slot_count, dtype=jnp.int32)
    key = block_offset * slot_count + index
    same = owner[:, None] == owner[None, :]
    earlier = same & (key[None, :] < key[:, None])
    order = jnp.sum(earlier.astype(jnp.int32), axis=1)
    again = jnp.any(earlier & (block_offset[None, :] == block_offset[:, None]), axis=1).astype(jnp.int32)
    far = (owner // half_count != my_half).astype(jnp.int32)
    place = owner % half_count
    panel_blocks = panel_rows.reshape(local_blocks, size, width)
    lanes = -(-max(local_blocks, LANES) // LANES) * LANES

    def tables(group):
        landing = (me % half_count) * per_owner + order
        cell = (group[None, :] == jnp.arange(2 * half_count, dtype=jnp.int32)[:, None])[:, None, :] & (
            block_offset[None, :] == jnp.arange(lanes, dtype=jnp.int32)[:, None]
        )[None]
        table = jnp.max(jnp.where(cell, landing[None, None, :], -1), axis=2)
        return jnp.where(table < 0, half_slots, table).reshape(2, half_count, 1, lanes)

    def whole():
        group = far * half_count + owner % half_count
        position = group * per_owner + order
        hit = position[None, :] == jnp.arange(2 * half_slots, dtype=jnp.int32)[:, None]
        pick = lambda value: jnp.max(jnp.where(hit, value[None, :], 0), axis=1)
        pair = tables(group).transpose(1, 0, 2, 3)
        pair = jnp.broadcast_to(pair, (half_count, 2, TILE, lanes)).reshape(half_count, 2 * TILE, lanes)
        return route(
            pick(index), pick(block_row), pick(again), sparse_blocks, panel_blocks, pair, row_half, per_owner
        )

    lower = min(2, row_half)
    around = lower * lax.axis_size("col")
    if half_count != 2 * around or local_blocks < 8:
        return whole().reshape(local_blocks * size, width)

    first_list = around // 2 * per_owner
    list_slots = max(slot_count // 2, first_list + 8)
    place = jnp.where(far == 1, (place + around) % half_count, place)
    table = tables(far * half_count + place)
    beyond = place // around != (me % half_count) // around
    flat_place = place % around
    listed = beyond & ((far == 0) | (flat_place % 2 == 1))
    list_group = jnp.where(far == 1, flat_place // 2, around // 2 + flat_place)
    list_group = jnp.where(listed, list_group, lanes)
    ahead = jnp.sum((list_group[None, :] < list_group[:, None]).astype(jnp.int32), axis=1)
    starts = jnp.sum(
        (list_group[None, :] < jnp.arange(lanes, dtype=jnp.int32)[:, None]).astype(jnp.int32), axis=1
    )
    spilled = jnp.sum(listed.astype(jnp.int32)) > list_slots
    starts = jnp.where(jnp.arange(lanes) == lanes - 1, jnp.where(spilled, SPILL, 0), starts)
    list_base = around * per_owner + half_slots
    position = jnp.where(
        listed,
        list_base + ahead + order,
        jnp.where(far == 1, around * per_owner + place * per_owner + order, flat_place * per_owner + order),
    )
    packed = (index * local_blocks + block_row) * 2 + again
    hit = position[None, :] == jnp.arange(list_base + list_slots, dtype=jnp.int32)[:, None]
    slots = jnp.max(jnp.where(hit, packed[None, :], 0), axis=1)
    kind = jnp.arange(TILE, dtype=jnp.int32)[None, :, None]
    rows = jnp.where(kind == 0, table[0], jnp.where(kind == 1, table[1], starts[None, None, :]))
    total, flags = route_layers(
        slots, sparse_blocks, panel_blocks, rows, row_half, per_owner, first_list, list_slots
    )
    total = lax.cond(flags[0, 0] >= SPILL, whole, lambda: total)
    return total.reshape(local_blocks * size, width)


def solution(mesh):
    placed = (
        P(AXES, None, None),
        P(AXES, None),
        P(AXES),
        P(AXES, None),
        P(AXES),
    )
    return jax.shard_map(
        body, mesh=mesh, in_specs=placed, out_specs=P(AXES, None), check_vma=False
    )
```

```python
import functools

import jax
import jax.numpy as jnp
from jax import lax
from jax.experimental import pallas as pl
from jax.experimental.pallas import tpu as pltpu
from jax.sharding import PartitionSpec as P

AXES = ("row", "col")
VMEM_LIMIT = 67_000_000
LANES = 128
TILE = 8
MESH = pl.DeviceIdType.MESH


def split_parts(value):
    high = value.astype(jnp.bfloat16)
    low = (value - high.astype(jnp.float32)).astype(jnp.bfloat16)
    return high, low


def block_product(block, panel):
    block_high, block_low = split_parts(block)
    panel_high, panel_low = split_parts(panel)
    dims = (((0,), (0,)), ((), ()))
    dot = functools.partial(lax.dot_general, dimension_numbers=dims, preferred_element_type=jnp.float32)
    return dot(
        jnp.concatenate([block_high, block_low], axis=0),
        jnp.concatenate([panel_high, panel_high], axis=0),
    ) + dot(block_high, panel_low)


def peers_of(upper, lower, outer):
    moves = [
        (a, b, c) for a in range(upper) for b in range(lower) for c in range(outer) if (a, b, c) != (0, 0, 0)
    ]
    single = [move for move in moves if sum(digit > 0 for digit in move) == 1]
    double = [move for move in moves if sum(digit > 0 for digit in move) == 2]
    zeros = lambda move: tuple(digit == 0 for digit in move)
    order = sorted(single, key=zeros)
    opposite = sorted(double, key=lambda move: tuple(digit > 0 for digit in move))
    pairs = list(zip(order, opposite))
    first = [one for one, _ in pairs] + [other for _, other in pairs]
    second = [other for _, other in pairs] + [one for one, _ in pairs]
    rest = [move for move in moves if move not in first]
    return first + rest, second + rest


def route_kernel(
    row_half,
    per_owner,
    source_ref,
    panel_at_ref,
    keep_ref,
    sparse_hbm,
    panel_hbm,
    table_hbm,
    out_hbm,
    sparse,
    panel,
    products,
    far_land,
    near_land,
    sums,
    crossed,
    total,
    tables,
    near_table,
    far_table,
    data_send,
    data_recv,
    table_send,
    table_recv,
    cross_send,
    cross_recv,
    load_sems,
    own_sems,
    out_sems,
):
    row, col = lax.axis_index("row"), lax.axis_index("col")
    row_count, col_count = lax.axis_size("row"), lax.axis_size("col")
    half, inner = row // row_half, row % row_half
    outer, core = col // 2, col % 2
    lower = min(2, row_half)
    mine = inner * col_count + col
    count = row_half * col_count
    half_slots = count * per_owner
    upper_count, outer_count = row_half // lower, col_count // 2
    local_blocks = total.shape[0]
    chunk = min(8, local_blocks)
    chunks = local_blocks // chunk

    loads = [
        pltpu.make_async_copy(sparse_hbm, sparse, load_sems.at[0]),
        pltpu.make_async_copy(panel_hbm, panel, load_sems.at[1]),
    ]
    for load in loads:
        load.start()
    blank = jnp.zeros(far_land.shape[1:], jnp.float32)
    far_land[half_slots] = blank
    near_land[half_slots] = blank

    def target(move_pair, flip):
        one, other = move_pair
        a, b, c = (x + core * (y - x) for x, y in zip(one, other))
        there = (inner // lower + a) % upper_count * lower + (inner % lower + b) % lower
        beside = (outer + c) % outer_count * 2 + (core + flip) % 2
        number = ((a * lower + b) * outer_count + c) * 2 + flip
        return (half * row_half + there, beside), there * col_count + beside, number

    firsts, seconds = peers_of(upper_count, lower, outer_count)
    moves = list(zip(firsts, seconds))
    still = ((0, 0, 0), (0, 0, 0))
    targets = [target(move, (core + phase) % 2) for phase in range(2) for move in moves]
    targets.append(target(still, 1))
    opposite = ((row + row_half) % row_count, col)

    barrier = pltpu.get_barrier_semaphore()
    for device, _, _ in targets:
        pl.semaphore_signal(barrier, inc=1, device_id=device, device_id_type=MESH)
    pl.semaphore_signal(barrier, inc=1, device_id=opposite, device_id_type=MESH)
    pl.semaphore_wait(barrier, len(targets) + 1)

    def remote(source, destination, send_sem, recv_sem, device):
        copy = pltpu.make_async_remote_copy(
            src_ref=source,
            dst_ref=destination,
            send_sem=send_sem,
            recv_sem=recv_sem,
            device_id=device,
            device_id_type=MESH,
        )
        copy.start()
        return copy

    table_copies = [
        remote(table_hbm.at[place], tables.at[mine], table_send.at[number], table_recv.at[number], device)
        for device, place, number in targets
    ]
    own_table = pltpu.make_async_copy(table_hbm.at[mine], tables.at[mine], own_sems.at[0])
    own_table.start()
    for load in loads:
        load.wait()

    unit = min(4, per_owner)

    def fill(base, place, destination, at):
        first = base + place * per_owner

        def some(step, _):
            for k in range(unit):
                slot = step * unit + k
                source = source_ref[first + slot]
                product = block_product(sparse[source], panel[panel_at_ref[first + slot]])
                before = destination[at + jnp.maximum(slot - 1, 0)]
                product = product + jnp.where(keep_ref[first + slot] > 0, before, 0.0)
                destination[at + slot] = product
            return 0

        lax.fori_loop(0, per_owner // unit, some, 0)

    def spread(base, land, shift):
        copies = []
        for device, place, number in targets:
            at = base + place * per_owner
            fill(base, place, products, at)
            copies.append(
                remote(
                    products.at[pl.ds(at, per_owner)],
                    land.at[pl.ds(mine * per_owner, per_owner)],
                    data_send.at[shift + number],
                    data_recv.at[shift + number],
                    device,
                )
            )
        fill(base, mine, land, mine * per_owner)
        return copies

    far_copies = spread(half_slots, far_land, count)
    near_copies = spread(0, near_land, 0)

    own_table.wait()
    for copy in table_copies:
        copy.wait_recv()
    lookups = [
        pltpu.make_async_copy(tables.at[:, 0, :], near_table, own_sems.at[1]),
        pltpu.make_async_copy(tables.at[:, TILE, :], far_table, own_sems.at[2]),
    ]
    for lookup in lookups:
        lookup.start()
    for lookup in lookups:
        lookup.wait()

    def reduce(land, table, destination, first, number):
        def one(step, _):
            column = first + step
            value = land[table[0, column]]
            for origin in range(1, count):
                value = value + land[table[origin, column]]
            destination[column] = value
            return 0

        lax.fori_loop(0, number, one, 0)

    for copy in far_copies:
        copy.wait_recv()
    cross_copies = []
    for index in range(chunks):
        reduce(far_land, far_table, sums, index * chunk, chunk)
        part = pl.ds(index * chunk, chunk)
        cross_copies.append(
            remote(sums.at[part], crossed.at[part], cross_send.at[index], cross_recv.at[index], opposite)
        )
    for copy in near_copies:
        copy.wait_recv()
    reduce(near_land, near_table, total, 0, local_blocks)
    outs = []
    for index, copy in enumerate(cross_copies):
        copy.wait_recv()
        part = pl.ds(index * chunk, chunk)
        total[part] = total[part] + crossed[part]
        out = pltpu.make_async_copy(total.at[part], out_hbm.at[part], out_sems.at[index])
        out.start()
        outs.append(out)
    for copy in table_copies + far_copies + near_copies + cross_copies:
        copy.wait_send()
    for out in outs:
        out.wait()


def route(source, panel_at, keep, sparse_blocks, panel_blocks, table, row_half, per_owner):
    count = row_half * lax.axis_size("col")
    local_blocks, size, width = panel_blocks.shape
    half_slots = count * per_owner
    chunks = local_blocks // min(8, local_blocks)
    lanes = table.shape[-1]
    scalars = pl.BlockSpec(memory_space=pltpu.SMEM)
    anywhere = pl.BlockSpec(memory_space=pl.ANY)
    block = (size, width)
    dma = pltpu.SemaphoreType.DMA
    return pl.pallas_call(
        functools.partial(route_kernel, row_half, per_owner),
        in_specs=[scalars] * 3 + [anywhere] * 3,
        out_specs=anywhere,
        out_shape=jax.ShapeDtypeStruct((local_blocks,) + block, jnp.float32),
        scratch_shapes=[
            pltpu.VMEM(sparse_blocks.shape, jnp.float32),
            pltpu.VMEM(panel_blocks.shape, jnp.float32),
            pltpu.VMEM((2 * half_slots,) + block, jnp.float32),
            pltpu.VMEM((half_slots + 1,) + block, jnp.float32),
            pltpu.VMEM((half_slots + 1,) + block, jnp.float32),
            pltpu.VMEM((local_blocks,) + block, jnp.float32),
            pltpu.VMEM((local_blocks,) + block, jnp.float32),
            pltpu.VMEM((local_blocks,) + block, jnp.float32),
            pltpu.VMEM((count, 2 * TILE, lanes), jnp.int32),
            pltpu.SMEM((count, lanes), jnp.int32),
            pltpu.SMEM((count, lanes), jnp.int32),
            dma((2 * count,)),
            dma((2 * count,)),
            dma((count,)),
            dma((count,)),
            dma((chunks,)),
            dma((chunks,)),
            dma((2,)),
            dma((3,)),
            dma((chunks,)),
        ],
        compiler_params=pltpu.CompilerParams(
            collective_id=0, has_side_effects=True, vmem_limit_bytes=VMEM_LIMIT
        ),
    )(source, panel_at, keep, sparse_blocks, panel_blocks, table)


def prepare(items_ref, made, slots_made, half, mine, per_owner, count, around, local_blocks, list_slots):
    slots = items_ref.shape[1]
    across = jnp.broadcast_to(items_ref[...], (slots, slots))
    down = jnp.transpose(across)
    lane = lax.broadcasted_iota(jnp.int32, (slots, LANES), 1)
    item = lax.broadcasted_iota(jnp.int32, (slots, LANES), 0)
    half_slots = count * per_owner

    def parts(packed):
        offset = packed // local_blocks % local_blocks
        owner = packed // (local_blocks * local_blocks)
        far = owner // count != half
        place = jnp.where(far, (owner + around) % count, owner % count)
        flat = place % around
        listed = (place // around != mine // around) & (jnp.logical_not(far) | (flat % 2 == 1))
        list_group = jnp.where(listed, jnp.where(far, flat // 2, around // 2 + flat), LANES)
        return owner, offset, far, place, flat, listed, list_group

    owner_r, offset_r, _, _, _, _, list_group_r = parts(across)
    owner_c, offset_c, far_c, place_c, flat_c, listed_c, list_group_c = parts(down)
    key_r, key_c = offset_r * slots + lane, offset_c * slots + item
    earlier = (owner_r == owner_c) & (key_r < key_c)
    total = lambda mask, value: jnp.sum(jnp.where(mask, value, 0), axis=1, keepdims=True)
    ranked = total(earlier, jnp.where(offset_r == offset_c, slots + 1, 1))
    order, again = jnp.minimum(ranked % slots, per_owner - 1), jnp.minimum(ranked // slots, 1)
    ahead = total(list_group_r < list_group_c, 1)
    position = jnp.where(
        listed_c,
        around * per_owner + half_slots + ahead + order,
        jnp.where(far_c, around * per_owner + place_c * per_owner + order, flat_c * per_owner + order),
    )
    packed = (item * local_blocks + down % local_blocks) * 2 + again
    for block in range(slots_made.shape[0]):
        picked = jnp.max(jnp.where(position == lane + block * LANES, packed, 0), axis=0, keepdims=True)
        slots_made[pl.ds(block, 1), :] = picked
    starts = jnp.sum((list_group_c < lane).astype(jnp.int32), axis=0, keepdims=True)
    landing = jnp.where(offset_c == lane, mine * per_owner + order, -1)
    kind = lax.broadcasted_iota(jnp.int32, (TILE, LANES), 0)

    def table(far, index):
        own = (far_c == far) & (place_c == index)
        best = jnp.max(jnp.where(own, landing, -1), axis=0, keepdims=True)
        return jnp.where(best < 0, half_slots, best)

    for index in range(count):
        near, away = table(False, index), table(True, index)
        made[index] = jnp.where(kind == 0, near, jnp.where(kind == 1, away, starts))


def layer_kernel(
    row_half,
    per_owner,
    first_list,
    items_ref,
    sparse_hbm,
    panel_hbm,
    out_hbm,
    flag_ref,
    sparse,
    panel,
    products,
    far_land,
    near_land,
    list_one,
    list_two,
    sums,
    crossed,
    total,
    tables,
    made,
    slots_made,
    slot_ref,
    spill,
    spill_in,
    near_table,
    far_table,
    starts,
    far_send,
    far_recv,
    near_send,
    near_recv,
    pass_send,
    pass_recv,
    list_send,
    list_recv,
    table_send,
    table_recv,
    cross_send,
    cross_recv,
    spill_sems,
    load_sems,
    own_sems,
    out_sems,
    beside_sems,
    across_sems,
):
    row, col = lax.axis_index("row"), lax.axis_index("col")
    col_count = lax.axis_size("col")
    half, inner = row // row_half, row % row_half
    outer, core = col // 2, col % 2
    lower = min(2, row_half)
    layer, beside_x = inner // lower, inner % lower
    mine = inner * col_count + col
    count = row_half * col_count
    around = lower * col_count
    half_slots = count * per_owner
    outer_count = col_count // 2
    rows_of_panel = panel.shape[0]
    local_blocks = total.shape[0]
    chunk = min(8, local_blocks)
    chunks = local_blocks // chunk
    second_list = list_two.shape[0]
    near_base, far_base, list_base = 0, around * per_owner, around * per_owner + half_slots

    loads = [
        pltpu.make_async_copy(sparse_hbm, sparse, load_sems.at[0]),
        pltpu.make_async_copy(panel_hbm, panel, load_sems.at[1]),
    ]
    for load in loads:
        load.start()
    blank = jnp.zeros(far_land.shape[1:], jnp.float32)
    far_land[half_slots] = blank
    near_land[half_slots] = blank

    def target(move_pair, flip):
        one, other = move_pair
        a, b, c = (x + core * (y - x) for x, y in zip(one, other))
        there = (layer + a) % 2 * lower + (beside_x + b) % lower
        beside = (outer + c) % outer_count * 2 + (core + flip) % 2
        number = ((a * lower + b) * outer_count + c) * 2 + flip
        return (half * row_half + there, beside), there * col_count + beside, number

    firsts, seconds = peers_of(2, lower, outer_count)
    moves = list(zip(firsts, seconds))
    flat = [move for move in firsts if move[0] == 0]
    flat_moves = list(zip(flat, sorted(flat, key=lambda move: (sum(move), move[1]))))
    still = ((0, 0, 0), (0, 0, 0))
    sibling = target(still, 1)
    partner_inner = (layer + 1) % 2 * lower + beside_x
    partner, partner_place = (half * row_half + partner_inner, col), partner_inner * col_count + col
    opposite = ((1 - half) * row_half + (1 - layer) * lower + beside_x, col)

    everyone = [target(move, (core + phase) % 2) for phase in range(2) for move in moves] + [sibling]
    barrier = pltpu.get_barrier_semaphore()
    for device, _, _ in everyone:
        pl.semaphore_signal(barrier, inc=1, device_id=device, device_id_type=MESH)
    pl.semaphore_signal(barrier, inc=1, device_id=opposite, device_id_type=MESH)

    with jax.named_scope("prepare"):
        prepare(
            items_ref, made, slots_made, half, mine, per_owner, count, around, local_blocks, first_list + second_list
        )
        slot_copy = pltpu.make_async_copy(slots_made, slot_ref, own_sems.at[4])
        slot_copy.start()
    with jax.named_scope("barrier"):
        pl.semaphore_wait(barrier, len(everyone) + 1)

    def remote(source, destination, send_sem, recv_sem, device):
        return pltpu.make_async_remote_copy(
            src_ref=source,
            dst_ref=destination,
            send_sem=send_sem,
            recv_sem=recv_sem,
            device_id=device,
            device_id_type=MESH,
        )

    def begin(copy):
        copy.start()
        return copy

    table_copies = [
        begin(remote(made.at[place], tables.at[mine], table_send.at[number], table_recv.at[number], device))
        for device, place, number in everyone
    ]
    own_table = pltpu.make_async_copy(made.at[mine], tables.at[mine], own_sems.at[0])
    own_table.start()
    slot_copy.wait()
    with jax.named_scope("load_wait"):
        for load in loads:
            load.wait()

    def fill(base, slots, destination, at, lead=0):
        unit = min(4, slots)

        def some(step, _):
            for k in range(unit):
                slot = step * unit + k
                packed = slot_ref[(base + slot) // LANES, (base + slot) % LANES]
                source, panel_at = packed // (2 * rows_of_panel), packed // 2 % rows_of_panel
                product = block_product(sparse[source], panel[panel_at])
                before = destination[at + jnp.maximum(slot - 1, -lead)]
                destination[at + slot] = product + jnp.where(packed % 2 > 0, before, 0.0)
            return 0

        lax.fori_loop(0, slots // unit, some, 0)

    def direct(base, index, land, send, recv, number, device, later=False):
        at = base + index * per_owner
        copy = remote(
            products.at[pl.ds(at, per_owner)],
            land.at[pl.ds(mine * per_owner, per_owner)],
            send.at[number],
            recv.at[number],
            device,
        )

        fill(at, per_owner, products, at)
        if not later:
            copy.start()
        return copy

    def send_far(device, place, number):
        return direct(far_base, place, far_land, far_send, far_recv, number, device)

    def send_near(device, place, number):
        return direct(near_base, place % around, near_land, near_send, near_recv, number, device, True)

    def send_list(first, land, index):
        slots = land.shape[0]
        fill(list_base + first, slots, products, list_base + first, min(first, 1))
        return remote(
            products.at[pl.ds(list_base + first, slots)], land, list_send.at[index], list_recv.at[index], partner
        )

    with jax.named_scope("far_first"):
        far_copies = [send_far(*target(move, core)) for move in moves]
    with jax.named_scope("list_one"):
        list_one_copy = begin(send_list(0, list_one, 0))
    with jax.named_scope("far_second"):
        far_copies += [send_far(*target(move, (core + 1) % 2)) for move in flat_moves]
        far_copies.append(send_far(*sibling))
        fill(far_base + mine * per_owner, per_owner, far_land, mine * per_owner)
    with jax.named_scope("list_two"):
        list_two_copy = send_list(first_list, list_two, 1)

    at_end = layer == half

    near_targets = [target(move, (core + phase) % 2) for phase in range(2) for move in flat_moves] + [sibling]
    with jax.named_scope("near_own"):
        near_copies = [send_near(*one) for one in near_targets]
        fill(near_base + mine % around * per_owner, per_owner, near_land, mine * per_owner)

    def start_near():
        for copy in near_copies:
            copy.start()

    with jax.named_scope("table_wait"):
        own_table.wait()
        for copy in table_copies:
            copy.wait_recv()
    lookups = [
        pltpu.make_async_copy(tables.at[:, 0, :], near_table, own_sems.at[1]),
        pltpu.make_async_copy(tables.at[:, 1, :], far_table, own_sems.at[2]),
        pltpu.make_async_copy(tables.at[:, 2, :], starts, own_sems.at[3]),
    ]
    for lookup in lookups:
        lookup.start()
    worst = tables[0]
    for origin in range(1, count):
        worst = jnp.maximum(worst, tables[origin])
    spill[...] = worst
    spill_copy = begin(remote(spill, spill_in, spill_sems.at[0], spill_sems.at[1], opposite))
    for lookup in lookups:
        lookup.wait()

    def reduce(land, table, destination, first, number):
        def one(step, _):
            column = first + step
            value = land[table[0, column]]
            for origin in range(1, count):
                value = value + land[table[origin, column]]
            destination[column] = value
            return 0

        lax.fori_loop(0, number, one, 0)

    cross_copies = [
        remote(
            sums.at[pl.ds(index * chunk, chunk)],
            crossed.at[pl.ds(index * chunk, chunk)],
            cross_send.at[index],
            cross_recv.at[index],
            opposite,
        )
        for index in range(chunks)
    ]

    def cross(held=False):
        for index in range(chunks):
            reduce(far_land, far_table, sums, index * chunk, chunk)
            if not held:
                cross_copies[index].start()

    straight = [target(move, (core + phase) % 2) for phase in range(2) for move in flat_moves] + [sibling]
    level = lambda number, recv: remote(
        products.at[pl.ds(0, per_owner)],
        far_land.at[pl.ds(mine * per_owner, per_owner)],
        far_send.at[0],
        recv.at[number],
        partner,
    )

    def await_level():
        for _, _, number in straight:
            level(number, far_recv).wait_recv()

    @pl.when(core == 0)
    def _():
        with jax.named_scope("far_wait"):
            await_level()
            for number in range(around, count):
                level(number, far_recv).wait_recv()
        @pl.when(at_end)
        def _():
            with jax.named_scope("cross_early"):
                cross(True)

        @pl.when(jnp.logical_not(at_end))
        def _():
            with jax.named_scope("cross_early"):
                cross()

    def relay(index, starting, land, shift, both):
        def pull(place, destination, at):
            start = starts[partner_place, starting(place % around)]

            def one(k, _):
                where = start + k
                value = list_one[jnp.minimum(where, first_list - 1)]
                if both:
                    other = list_two[jnp.clip(where - first_list, 0, second_list - 1)]
                    value = jnp.where(where < first_list, value, other)
                destination[at + k] = value
                return 0

            lax.fori_loop(0, per_owner, one, 0)

        def push(device, place, number):
            at = shift + place % around * per_owner
            pull(place, sparse, at)
            return begin(
                remote(
                    sparse.at[pl.ds(at, per_owner)],
                    land.at[pl.ds(partner_place * per_owner, per_owner)],
                    pass_send.at[index * around + number],
                    pass_recv.at[index * around + number],
                    device,
                )
            )

        def keep():
            pull(mine, land, partner_place * per_owner)

        return push, keep

    push_far, keep_far = relay(0, lambda place: place // 2, far_land, 0, False)
    push_near, keep_near = relay(
        1, lambda place: around // 2 + place, near_land, around * per_owner, True
    )
    sibling_pass = lambda index, land: remote(
        sparse.at[pl.ds(0, per_owner)],
        land.at[pl.ds(partner_place * per_owner, per_owner)],
        pass_send.at[index * around + 1],
        pass_recv.at[index * around + 1],
        sibling[0],
    )

    with jax.named_scope("list_one_wait"):
        list_one_copy.wait_recv()

    @pl.when(jnp.logical_not(at_end))
    def _():
        list_two_copy.start()
    with jax.named_scope("pass_far"):
        far_passes = [push_far(*target(move, (core + 1) % 2)) for move in flat_moves]

    @pl.when(core == 0)
    def _():
        push_far(*sibling)

    @pl.when(at_end & (core == 1))
    def _():
        pl.semaphore_signal(beside_sems.at[0], inc=1, device_id=sibling[0], device_id_type=MESH)

    @pl.when(at_end & (core == 0))
    def _():
        pl.semaphore_wait(beside_sems.at[0], 1)
        pl.semaphore_signal(across_sems.at[0], inc=1, device_id=opposite, device_id_type=MESH)
        pl.semaphore_wait(across_sems.at[0], 1)
        for copy in cross_copies:
            copy.start()
        list_two_copy.start()

    start_near()

    @pl.when(core == 1)
    def _():
        keep_far()
        with jax.named_scope("pass_far_wait"):
            await_level()
            for _, _, number in straight:
                level(number, pass_recv).wait_recv()

        @pl.when(at_end)
        def _():
            list_two_copy.start()
            with jax.named_scope("cross_late"):
                cross(True)

        @pl.when(jnp.logical_not(at_end))
        def _():
            with jax.named_scope("cross_late"):
                cross()

    with jax.named_scope("list_two_wait"):
        list_two_copy.wait_recv()
    with jax.named_scope("pass_near"):
        near_passes = [push_near(*one) for one in near_targets]
        keep_near()

    @pl.when(at_end & (core == 0))
    def _():
        pl.semaphore_signal(beside_sems.at[1], inc=1, device_id=sibling[0], device_id_type=MESH)

    @pl.when(at_end & (core == 1))
    def _():
        pl.semaphore_wait(beside_sems.at[1], 1)
        pl.semaphore_signal(across_sems.at[1], inc=1, device_id=opposite, device_id_type=MESH)
        pl.semaphore_wait(across_sems.at[1], 1)
        for copy in cross_copies:
            copy.start()


    spill_copy.wait()
    spill[...] = jnp.maximum(spill[...], spill_in[...])
    flag_copy = pltpu.make_async_copy(spill.at[2], starts.at[0], own_sems.at[0])
    flag_copy.start()
    flag_copy.wait()
    flag_ref[0, 0] = starts[0, starts.shape[1] - 1]
    with jax.named_scope("near_wait"):
        for copy in near_copies + near_passes:
            copy.wait_recv()
    with jax.named_scope("near_sum"):
        reduce(near_land, near_table, total, 0, local_blocks)
    outs = []
    for index, copy in enumerate(cross_copies):
        with jax.named_scope(f"cross_wait{index}"):
            copy.wait_recv()
        part = pl.ds(index * chunk, chunk)
        total[part] = total[part] + crossed[part]
        out = pltpu.make_async_copy(total.at[part], out_hbm.at[part], out_sems.at[index])
        out.start()
        outs.append(out)
    sent = table_copies + far_copies + [list_one_copy, list_two_copy] + near_copies
    for copy in sent + far_passes + near_passes + cross_copies:
        copy.wait_send()

    @pl.when(core == 0)
    def _():
        sibling_pass(0, far_land).wait_send()

    for out in outs:
        out.wait()


def route_layers(items, sparse_blocks, panel_blocks, row_half, per_owner, first_list, list_slots):
    count = row_half * lax.axis_size("col")
    around = count // 2
    local_blocks, size, width = panel_blocks.shape
    half_slots = count * per_owner
    chunks = local_blocks // min(8, local_blocks)
    lanes = LANES
    made_slots = around * per_owner + half_slots + list_slots
    scalars = pl.BlockSpec(memory_space=pltpu.SMEM)
    anywhere = pl.BlockSpec(memory_space=pl.ANY)
    block = (size, width)
    dma = pltpu.SemaphoreType.DMA
    blocks = lambda number: pltpu.VMEM((number,) + block, jnp.float32)
    return pl.pallas_call(
        functools.partial(layer_kernel, row_half, per_owner, first_list),
        in_specs=[pl.BlockSpec(memory_space=pltpu.VMEM)] + [anywhere] * 2,
        out_specs=[anywhere, scalars],
        out_shape=[
            jax.ShapeDtypeStruct((local_blocks,) + block, jnp.float32),
            jax.ShapeDtypeStruct((1, 1), jnp.int32),
        ],
        scratch_shapes=[
            pltpu.VMEM(sparse_blocks.shape, jnp.float32),
            pltpu.VMEM(panel_blocks.shape, jnp.float32),
            blocks(around * per_owner + half_slots + list_slots),
            blocks(half_slots + 1),
            blocks(half_slots + 1),
            blocks(first_list),
            blocks(list_slots - first_list),
            blocks(local_blocks),
            blocks(local_blocks),
            blocks(local_blocks),
            pltpu.VMEM((count, TILE, lanes), jnp.int32),
            pltpu.VMEM((count, TILE, lanes), jnp.int32),
            pltpu.VMEM((-(-made_slots // lanes), lanes), jnp.int32),
            pltpu.SMEM((-(-made_slots // lanes), lanes), jnp.int32),
            pltpu.VMEM((TILE, lanes), jnp.int32),
            pltpu.VMEM((TILE, lanes), jnp.int32),
            pltpu.SMEM((count, lanes), jnp.int32),
            pltpu.SMEM((count, lanes), jnp.int32),
            pltpu.SMEM((count, lanes), jnp.int32),
            dma((count,)),
            dma((count,)),
            dma((around,)),
            dma((around,)),
            dma((2 * around,)),
            dma((2 * around,)),
            dma((2,)),
            dma((2,)),
            dma((count,)),
            dma((count,)),
            dma((chunks,)),
            dma((chunks,)),
            dma((2,)),
            dma((2,)),
            dma((5,)),
            dma((chunks,)),
            pltpu.SemaphoreType.REGULAR((2,)),
            pltpu.SemaphoreType.REGULAR((2,)),
        ],
        compiler_params=pltpu.CompilerParams(
            collective_id=1, has_side_effects=True, vmem_limit_bytes=VMEM_LIMIT
        ),
    )(items, sparse_blocks, panel_blocks)


def body(sparse_blocks, panel_rows, block_row, block_owner, block_offset):
    device_count = lax.axis_size("row") * lax.axis_size("col")
    half_count = device_count // 2
    slot_count, size, _ = sparse_blocks.shape
    width = panel_rows.shape[1]
    local_blocks = panel_rows.shape[0] // size
    per_owner = max(2, 2 * slot_count // device_count)
    half_slots = half_count * per_owner
    me = lax.axis_index(AXES)
    my_half = me // half_count
    row_half = lax.axis_size("row") // 2
    owner = block_owner[:, 0]
    panel_blocks = panel_rows.reshape(local_blocks, size, width)
    lanes = -(-max(local_blocks, LANES) // LANES) * LANES

    def whole():
        index = jnp.arange(slot_count, dtype=jnp.int32)
        key = block_offset * slot_count + index
        same = owner[:, None] == owner[None, :]
        earlier = same & (key[None, :] < key[:, None])
        order = jnp.sum(earlier.astype(jnp.int32), axis=1)
        again = jnp.any(earlier & (block_offset[None, :] == block_offset[:, None]), axis=1).astype(jnp.int32)
        far = (owner // half_count != my_half).astype(jnp.int32)
        group = far * half_count + owner % half_count
        landing = (me % half_count) * per_owner + order
        cell = (group[None, :] == jnp.arange(2 * half_count, dtype=jnp.int32)[:, None])[:, None, :] & (
            block_offset[None, :] == jnp.arange(lanes, dtype=jnp.int32)[:, None]
        )[None]
        table = jnp.max(jnp.where(cell, landing[None, None, :], -1), axis=2)
        table = jnp.where(table < 0, half_slots, table).reshape(2, half_count, 1, lanes)
        position = group * per_owner + order
        hit = position[None, :] == jnp.arange(2 * half_slots, dtype=jnp.int32)[:, None]
        pick = lambda value: jnp.max(jnp.where(hit, value[None, :], 0), axis=1)
        pair = table.transpose(1, 0, 2, 3)
        pair = jnp.broadcast_to(pair, (half_count, 2, TILE, lanes)).reshape(half_count, 2 * TILE, lanes)
        return route(
            pick(index), pick(block_row), pick(again), sparse_blocks, panel_blocks, pair, row_half, per_owner
        )

    lower = min(2, row_half)
    around = lower * lax.axis_size("col")
    if half_count != 2 * around or slot_count != LANES or not 8 <= local_blocks < LANES:
        return whole().reshape(local_blocks * size, width)

    first_list = around // 2 * per_owner
    list_slots = max(slot_count // 2, first_list + 8)
    items = ((owner * local_blocks + block_offset) * local_blocks + block_row).reshape(1, slot_count)
    total, flags = route_layers(items, sparse_blocks, panel_blocks, row_half, per_owner, first_list, list_slots)
    total = lax.cond(flags[0, 0] > list_slots, whole, lambda: total)
    return total.reshape(local_blocks * size, width)


def solution(mesh):
    placed = (
        P(AXES, None, None),
        P(AXES, None),
        P(AXES),
        P(AXES, None),
        P(AXES),
    )
    return jax.shard_map(
        body, mesh=mesh, in_specs=placed, out_specs=P(AXES, None), check_vma=False
    )
```

```python
import functools

import jax
import jax.numpy as jnp
from jax import lax
from jax.experimental import pallas as pl
from jax.experimental.pallas import tpu as pltpu
from jax.sharding import PartitionSpec as P

AXES = ("row", "col")
VMEM_LIMIT = 67_000_000
LANES = 128
TILE = 8
MESH = pl.DeviceIdType.MESH


def split_parts(value):
    high = value.astype(jnp.bfloat16)
    low = (value - high.astype(jnp.float32)).astype(jnp.bfloat16)
    return high, low


def block_product(block, panel):
    block_high, block_low = split_parts(block)
    panel_high, panel_low = split_parts(panel)
    dims = (((0,), (0,)), ((), ()))
    dot = functools.partial(lax.dot_general, dimension_numbers=dims, preferred_element_type=jnp.float32)
    return dot(
        jnp.concatenate([block_high, block_low], axis=0),
        jnp.concatenate([panel_high, panel_high], axis=0),
    ) + dot(block_high, panel_low)


def peers_of(upper, lower, outer):
    moves = [
        (a, b, c) for a in range(upper) for b in range(lower) for c in range(outer) if (a, b, c) != (0, 0, 0)
    ]
    single = [move for move in moves if sum(digit > 0 for digit in move) == 1]
    double = [move for move in moves if sum(digit > 0 for digit in move) == 2]
    zeros = lambda move: tuple(digit == 0 for digit in move)
    order = sorted(single, key=zeros)
    opposite = sorted(double, key=lambda move: tuple(digit > 0 for digit in move))
    pairs = list(zip(order, opposite))
    first = [one for one, _ in pairs] + [other for _, other in pairs]
    second = [other for _, other in pairs] + [one for one, _ in pairs]
    rest = [move for move in moves if move not in first]
    return first + rest, second + rest


def route_kernel(
    row_half,
    per_owner,
    source_ref,
    panel_at_ref,
    keep_ref,
    sparse_hbm,
    panel_hbm,
    table_hbm,
    out_hbm,
    sparse,
    panel,
    products,
    far_land,
    near_land,
    sums,
    crossed,
    total,
    tables,
    near_table,
    far_table,
    data_send,
    data_recv,
    table_send,
    table_recv,
    cross_send,
    cross_recv,
    load_sems,
    own_sems,
    out_sems,
):
    row, col = lax.axis_index("row"), lax.axis_index("col")
    row_count, col_count = lax.axis_size("row"), lax.axis_size("col")
    half, inner = row // row_half, row % row_half
    outer, core = col // 2, col % 2
    lower = min(2, row_half)
    mine = inner * col_count + col
    count = row_half * col_count
    half_slots = count * per_owner
    upper_count, outer_count = row_half // lower, col_count // 2
    local_blocks = total.shape[0]
    chunk = min(8, local_blocks)
    chunks = local_blocks // chunk

    loads = [
        pltpu.make_async_copy(sparse_hbm, sparse, load_sems.at[0]),
        pltpu.make_async_copy(panel_hbm, panel, load_sems.at[1]),
    ]
    for load in loads:
        load.start()
    blank = jnp.zeros(far_land.shape[1:], jnp.float32)
    far_land[half_slots] = blank
    near_land[half_slots] = blank

    def target(move_pair, flip):
        one, other = move_pair
        a, b, c = (x + core * (y - x) for x, y in zip(one, other))
        there = (inner // lower + a) % upper_count * lower + (inner % lower + b) % lower
        beside = (outer + c) % outer_count * 2 + (core + flip) % 2
        number = ((a * lower + b) * outer_count + c) * 2 + flip
        return (half * row_half + there, beside), there * col_count + beside, number

    firsts, seconds = peers_of(upper_count, lower, outer_count)
    moves = list(zip(firsts, seconds))
    still = ((0, 0, 0), (0, 0, 0))
    targets = [target(move, (core + phase) % 2) for phase in range(2) for move in moves]
    targets.append(target(still, 1))
    opposite = ((row + row_half) % row_count, col)

    barrier = pltpu.get_barrier_semaphore()
    for device, _, _ in targets:
        pl.semaphore_signal(barrier, inc=1, device_id=device, device_id_type=MESH)
    pl.semaphore_signal(barrier, inc=1, device_id=opposite, device_id_type=MESH)
    pl.semaphore_wait(barrier, len(targets) + 1)

    def remote(source, destination, send_sem, recv_sem, device):
        copy = pltpu.make_async_remote_copy(
            src_ref=source,
            dst_ref=destination,
            send_sem=send_sem,
            recv_sem=recv_sem,
            device_id=device,
            device_id_type=MESH,
        )
        copy.start()
        return copy

    table_copies = [
        remote(table_hbm.at[place], tables.at[mine], table_send.at[number], table_recv.at[number], device)
        for device, place, number in targets
    ]
    own_table = pltpu.make_async_copy(table_hbm.at[mine], tables.at[mine], own_sems.at[0])
    own_table.start()
    for load in loads:
        load.wait()

    unit = min(4, per_owner)

    def fill(base, place, destination, at):
        first = base + place * per_owner

        def some(step, _):
            for k in range(unit):
                slot = step * unit + k
                source = source_ref[first + slot]
                product = block_product(sparse[source], panel[panel_at_ref[first + slot]])
                before = destination[at + jnp.maximum(slot - 1, 0)]
                product = product + jnp.where(keep_ref[first + slot] > 0, before, 0.0)
                destination[at + slot] = product
            return 0

        lax.fori_loop(0, per_owner // unit, some, 0)

    def spread(base, land, shift):
        copies = []
        for device, place, number in targets:
            at = base + place * per_owner
            fill(base, place, products, at)
            copies.append(
                remote(
                    products.at[pl.ds(at, per_owner)],
                    land.at[pl.ds(mine * per_owner, per_owner)],
                    data_send.at[shift + number],
                    data_recv.at[shift + number],
                    device,
                )
            )
        fill(base, mine, land, mine * per_owner)
        return copies

    far_copies = spread(half_slots, far_land, count)
    near_copies = spread(0, near_land, 0)

    own_table.wait()
    for copy in table_copies:
        copy.wait_recv()
    lookups = [
        pltpu.make_async_copy(tables.at[:, 0, :], near_table, own_sems.at[1]),
        pltpu.make_async_copy(tables.at[:, TILE, :], far_table, own_sems.at[2]),
    ]
    for lookup in lookups:
        lookup.start()
    for lookup in lookups:
        lookup.wait()

    def reduce(land, table, destination, first, number):
        def one(step, _):
            column = first + step
            value = land[table[0, column]]
            for origin in range(1, count):
                value = value + land[table[origin, column]]
            destination[column] = value
            return 0

        lax.fori_loop(0, number, one, 0)

    for copy in far_copies:
        copy.wait_recv()
    cross_copies = []
    for index in range(chunks):
        reduce(far_land, far_table, sums, index * chunk, chunk)
        part = pl.ds(index * chunk, chunk)
        cross_copies.append(
            remote(sums.at[part], crossed.at[part], cross_send.at[index], cross_recv.at[index], opposite)
        )
    for copy in near_copies:
        copy.wait_recv()
    reduce(near_land, near_table, total, 0, local_blocks)
    outs = []
    for index, copy in enumerate(cross_copies):
        copy.wait_recv()
        part = pl.ds(index * chunk, chunk)
        total[part] = total[part] + crossed[part]
        out = pltpu.make_async_copy(total.at[part], out_hbm.at[part], out_sems.at[index])
        out.start()
        outs.append(out)
    for copy in table_copies + far_copies + near_copies + cross_copies:
        copy.wait_send()
    for out in outs:
        out.wait()


def route(source, panel_at, keep, sparse_blocks, panel_blocks, table, row_half, per_owner):
    count = row_half * lax.axis_size("col")
    local_blocks, size, width = panel_blocks.shape
    half_slots = count * per_owner
    chunks = local_blocks // min(8, local_blocks)
    lanes = table.shape[-1]
    scalars = pl.BlockSpec(memory_space=pltpu.SMEM)
    anywhere = pl.BlockSpec(memory_space=pl.ANY)
    block = (size, width)
    dma = pltpu.SemaphoreType.DMA
    return pl.pallas_call(
        functools.partial(route_kernel, row_half, per_owner),
        in_specs=[scalars] * 3 + [anywhere] * 3,
        out_specs=anywhere,
        out_shape=jax.ShapeDtypeStruct((local_blocks,) + block, jnp.float32),
        scratch_shapes=[
            pltpu.VMEM(sparse_blocks.shape, jnp.float32),
            pltpu.VMEM(panel_blocks.shape, jnp.float32),
            pltpu.VMEM((2 * half_slots,) + block, jnp.float32),
            pltpu.VMEM((half_slots + 1,) + block, jnp.float32),
            pltpu.VMEM((half_slots + 1,) + block, jnp.float32),
            pltpu.VMEM((local_blocks,) + block, jnp.float32),
            pltpu.VMEM((local_blocks,) + block, jnp.float32),
            pltpu.VMEM((local_blocks,) + block, jnp.float32),
            pltpu.VMEM((count, 2 * TILE, lanes), jnp.int32),
            pltpu.SMEM((count, lanes), jnp.int32),
            pltpu.SMEM((count, lanes), jnp.int32),
            dma((2 * count,)),
            dma((2 * count,)),
            dma((count,)),
            dma((count,)),
            dma((chunks,)),
            dma((chunks,)),
            dma((2,)),
            dma((3,)),
            dma((chunks,)),
        ],
        compiler_params=pltpu.CompilerParams(
            collective_id=0, has_side_effects=True, vmem_limit_bytes=VMEM_LIMIT
        ),
    )(source, panel_at, keep, sparse_blocks, panel_blocks, table)


def prepare(owner_ref, offset_ref, row_ref, made, slots_made, half, mine, per_owner, count, around, local_blocks, list_slots):
    slots = owner_ref.shape[1]
    items = (owner_ref[...] * local_blocks + offset_ref[...]) * local_blocks + row_ref[...]
    across = jnp.broadcast_to(items, (slots, slots))
    down = jnp.transpose(across)
    lane = lax.broadcasted_iota(jnp.int32, (slots, LANES), 1)
    item = lax.broadcasted_iota(jnp.int32, (slots, LANES), 0)
    half_slots = count * per_owner

    def parts(packed):
        offset = packed // local_blocks % local_blocks
        owner = packed // (local_blocks * local_blocks)
        far = owner // count != half
        place = jnp.where(far, (owner + around) % count, owner % count)
        flat = place % around
        listed = (place // around != mine // around) & (jnp.logical_not(far) | (flat % 2 == 1))
        list_group = jnp.where(listed, jnp.where(far, flat // 2, around // 2 + flat), LANES)
        return owner, offset, far, place, flat, listed, list_group

    owner_r, offset_r, _, _, _, _, list_group_r = parts(across)
    owner_c, offset_c, far_c, place_c, flat_c, listed_c, list_group_c = parts(down)
    key_r, key_c = offset_r * slots + lane, offset_c * slots + item
    earlier = (owner_r == owner_c) & (key_r < key_c)
    total = lambda mask, value: jnp.sum(jnp.where(mask, value, 0), axis=1, keepdims=True)
    ranked = total(earlier, jnp.where(offset_r == offset_c, slots + 1, 1))
    order, again = jnp.minimum(ranked % slots, per_owner - 1), jnp.minimum(ranked // slots, 1)
    ahead = total(list_group_r < list_group_c, 1)
    position = jnp.where(
        listed_c,
        around * per_owner + half_slots + ahead + order,
        jnp.where(far_c, around * per_owner + place_c * per_owner + order, flat_c * per_owner + order),
    )
    packed = (item * local_blocks + down % local_blocks) * 2 + again
    for block in range(slots_made.shape[0]):
        picked = jnp.max(jnp.where(position == lane + block * LANES, packed, 0), axis=0, keepdims=True)
        slots_made[pl.ds(block, 1), :] = picked
    starts = jnp.sum((list_group_c < lane).astype(jnp.int32), axis=0, keepdims=True)
    landing = jnp.where(offset_c == lane, mine * per_owner + order, -1)
    kind = lax.broadcasted_iota(jnp.int32, (TILE, LANES), 0)

    def table(far, index):
        own = (far_c == far) & (place_c == index)
        best = jnp.max(jnp.where(own, landing, -1), axis=0, keepdims=True)
        return jnp.where(best < 0, half_slots, best)

    for index in range(count):
        near, away = table(False, index), table(True, index)
        made[index] = jnp.where(kind == 0, near, jnp.where(kind == 1, away, starts))


def layer_kernel(
    row_half,
    per_owner,
    first_list,
    owner_ref,
    offset_ref,
    row_ref,
    sparse_hbm,
    panel_hbm,
    out_hbm,
    flag_ref,
    sparse,
    panel,
    products,
    far_land,
    near_own,
    near_pass,
    list_one,
    list_two,
    sums,
    crossed,
    total,
    tables,
    made,
    slots_made,
    slot_ref,
    spill,
    spill_in,
    near_table,
    far_table,
    starts,
    far_send,
    far_recv,
    near_send,
    near_recv,
    pass_send,
    pass_recv,
    list_send,
    list_recv,
    table_send,
    table_recv,
    cross_send,
    cross_recv,
    spill_sems,
    load_sems,
    own_sems,
    out_sems,
    beside_sems,
    across_sems,
):
    row, col = lax.axis_index("row"), lax.axis_index("col")
    col_count = lax.axis_size("col")
    half, inner = row // row_half, row % row_half
    outer, core = col // 2, col % 2
    lower = min(2, row_half)
    layer, beside_x = inner // lower, inner % lower
    mine = inner * col_count + col
    count = row_half * col_count
    around = lower * col_count
    half_slots = count * per_owner
    outer_count = col_count // 2
    rows_of_panel = panel.shape[0]
    local_blocks = total.shape[0]
    chunk = min(8, local_blocks)
    chunks = local_blocks // chunk
    second_list = list_two.shape[0]
    near_base, far_base, list_base = 0, around * per_owner, around * per_owner + half_slots

    loads = [
        pltpu.make_async_copy(sparse_hbm, sparse, load_sems.at[0]),
        pltpu.make_async_copy(panel_hbm, panel, load_sems.at[1]),
    ]
    for load in loads:
        load.start()
    blank = jnp.zeros(far_land.shape[1:], jnp.float32)
    far_land[half_slots] = blank
    near_own[around * per_owner] = blank
    near_pass[around * per_owner] = blank

    def target(move_pair, flip):
        one, other = move_pair
        a, b, c = (x + core * (y - x) for x, y in zip(one, other))
        there = (layer + a) % 2 * lower + (beside_x + b) % lower
        beside = (outer + c) % outer_count * 2 + (core + flip) % 2
        number = ((a * lower + b) * outer_count + c) * 2 + flip
        return (half * row_half + there, beside), there * col_count + beside, number

    firsts, seconds = peers_of(2, lower, outer_count)
    moves = list(zip(firsts, seconds))
    flat = [move for move in firsts if move[0] == 0]
    flat_moves = list(zip(flat, sorted(flat, key=lambda move: (sum(move), move[1]))))
    still = ((0, 0, 0), (0, 0, 0))
    sibling = target(still, 1)
    partner_inner = (layer + 1) % 2 * lower + beside_x
    partner, partner_place = (half * row_half + partner_inner, col), partner_inner * col_count + col
    opposite = ((1 - half) * row_half + (1 - layer) * lower + beside_x, col)

    everyone = [target(move, (core + phase) % 2) for phase in range(2) for move in moves] + [sibling]
    barrier = pltpu.get_barrier_semaphore()
    for device, _, _ in everyone:
        pl.semaphore_signal(barrier, inc=1, device_id=device, device_id_type=MESH)
    pl.semaphore_signal(barrier, inc=1, device_id=opposite, device_id_type=MESH)

    with jax.named_scope("prepare"):
        prepare(
            owner_ref,
            offset_ref,
            row_ref,
            made,
            slots_made,
            half,
            mine,
            per_owner,
            count,
            around,
            local_blocks,
            first_list + second_list,
        )
        slot_copy = pltpu.make_async_copy(slots_made, slot_ref, own_sems.at[4])
        slot_copy.start()
    with jax.named_scope("barrier"):
        pl.semaphore_wait(barrier, len(everyone) + 1)

    def remote(source, destination, send_sem, recv_sem, device):
        return pltpu.make_async_remote_copy(
            src_ref=source,
            dst_ref=destination,
            send_sem=send_sem,
            recv_sem=recv_sem,
            device_id=device,
            device_id_type=MESH,
        )

    def begin(copy):
        copy.start()
        return copy

    table_copies = [
        begin(remote(made.at[place], tables.at[mine], table_send.at[number], table_recv.at[number], device))
        for device, place, number in everyone
    ]
    own_table = pltpu.make_async_copy(made.at[mine], tables.at[mine], own_sems.at[0])
    own_table.start()
    slot_copy.wait()
    with jax.named_scope("load_wait"):
        for load in loads:
            load.wait()

    def fill(base, slots, destination, at, lead=0):
        unit = min(4, slots)

        def some(step, _):
            for k in range(unit):
                slot = step * unit + k
                packed = slot_ref[(base + slot) // LANES, (base + slot) % LANES]
                source, panel_at = packed // (2 * rows_of_panel), packed // 2 % rows_of_panel
                product = block_product(sparse[source], panel[panel_at])
                before = destination[at + jnp.maximum(slot - 1, -lead)]
                destination[at + slot] = product + jnp.where(packed % 2 > 0, before, 0.0)
            return 0

        lax.fori_loop(0, slots // unit, some, 0)

    def direct(base, index, land, spot, send, recv, number, device, later=False):
        at = base + index * per_owner
        copy = remote(
            products.at[pl.ds(at, per_owner)],
            land.at[pl.ds(spot * per_owner, per_owner)],
            send.at[number],
            recv.at[number],
            device,
        )

        fill(at, per_owner, products, at)
        if not later:
            copy.start()
        return copy

    def send_far(device, place, number):
        return direct(far_base, place, far_land, mine, far_send, far_recv, number, device)

    def send_near(device, place, number):
        return direct(near_base, place % around, near_own, mine % around, near_send, near_recv, number, device, True)

    def send_list(first, land, index):
        slots = land.shape[0]
        fill(list_base + first, slots, products, list_base + first, min(first, 1))
        return remote(
            products.at[pl.ds(list_base + first, slots)], land, list_send.at[index], list_recv.at[index], partner
        )

    with jax.named_scope("far_first"):
        far_copies = [send_far(*target(move, core)) for move in sorted(moves, key=lambda pair: -pair[0][0] - pair[1][0])]
    with jax.named_scope("list_one"):
        list_one_copy = begin(send_list(0, list_one, 0))
    with jax.named_scope("far_second"):
        far_copies += [send_far(*target(move, (core + 1) % 2)) for move in flat_moves]
        far_copies.append(send_far(*sibling))
        fill(far_base + mine * per_owner, per_owner, far_land, mine * per_owner)
    with jax.named_scope("list_two"):
        list_two_copy = send_list(first_list, list_two, 1)

    at_end = layer == half

    near_targets = [target(move, (core + phase) % 2) for phase in range(2) for move in flat_moves] + [sibling]
    with jax.named_scope("near_own"):
        near_copies = [send_near(*one) for one in near_targets]
        fill(near_base + mine % around * per_owner, per_owner, near_own, mine % around * per_owner)

    def start_near():
        for copy in near_copies:
            copy.start()

    with jax.named_scope("table_wait"):
        own_table.wait()
        for copy in table_copies:
            copy.wait_recv()
    lookups = [
        pltpu.make_async_copy(tables.at[:, 0, :], near_table, own_sems.at[1]),
        pltpu.make_async_copy(tables.at[:, 1, :], far_table, own_sems.at[2]),
        pltpu.make_async_copy(tables.at[:, 2, :], starts, own_sems.at[3]),
    ]
    for lookup in lookups:
        lookup.start()
    worst = tables[0]
    for origin in range(1, count):
        worst = jnp.maximum(worst, tables[origin])
    spill[...] = worst
    spill_copy = begin(remote(spill, spill_in, spill_sems.at[0], spill_sems.at[1], opposite))
    for lookup in lookups:
        lookup.wait()

    def reduce(land, table, destination, first, number):
        def one(step, _):
            column = first + step
            value = land[table[0, column]]
            for origin in range(1, count):
                value = value + land[table[origin, column]]
            destination[column] = value
            return 0

        lax.fori_loop(0, number, one, 0)

    cross_copies = [
        remote(
            sums.at[pl.ds(index * chunk, chunk)],
            crossed.at[pl.ds(index * chunk, chunk)],
            cross_send.at[index],
            cross_recv.at[index],
            opposite,
        )
        for index in range(chunks)
    ]

    def cross(held=False):
        for index in range(chunks):
            reduce(far_land, far_table, sums, index * chunk, chunk)
            if not held:
                cross_copies[index].start()

    straight = [target(move, (core + phase) % 2) for phase in range(2) for move in flat_moves] + [sibling]
    level = lambda number, recv: remote(
        products.at[pl.ds(0, per_owner)],
        far_land.at[pl.ds(mine * per_owner, per_owner)],
        far_send.at[0],
        recv.at[number],
        partner,
    )

    def await_level():
        for _, _, number in straight:
            level(number, far_recv).wait_recv()

    @pl.when(core == 0)
    def _():
        with jax.named_scope("far_wait"):
            await_level()
            for number in range(around, count):
                level(number, far_recv).wait_recv()
        @pl.when(at_end)
        def _():
            with jax.named_scope("cross_early"):
                cross(True)

        @pl.when(jnp.logical_not(at_end))
        def _():
            with jax.named_scope("cross_early"):
                cross()

    def relay(index, starting, land, spot, shift, both):
        def pull(place, destination, at):
            start = starts[partner_place, starting(place % around)]

            def one(k, _):
                where = start + k
                value = list_one[jnp.minimum(where, first_list - 1)]
                if both:
                    other = list_two[jnp.clip(where - first_list, 0, second_list - 1)]
                    value = jnp.where(where < first_list, value, other)
                destination[at + k] = value
                return 0

            lax.fori_loop(0, per_owner, one, 0)

        def push(device, place, number):
            at = shift + place % around * per_owner
            pull(place, sparse, at)
            return begin(
                remote(
                    sparse.at[pl.ds(at, per_owner)],
                    land.at[pl.ds(spot * per_owner, per_owner)],
                    pass_send.at[index * around + number],
                    pass_recv.at[index * around + number],
                    device,
                )
            )

        def keep():
            pull(mine, land, spot * per_owner)

        return push, keep

    push_far, keep_far = relay(0, lambda place: place // 2, far_land, partner_place, 0, False)
    push_near, keep_near = relay(
        1, lambda place: around // 2 + place, near_pass, mine % around, around * per_owner, True
    )
    sibling_pass = lambda index, land: remote(
        sparse.at[pl.ds(0, per_owner)],
        land.at[pl.ds(partner_place * per_owner, per_owner)],
        pass_send.at[index * around + 1],
        pass_recv.at[index * around + 1],
        sibling[0],
    )

    with jax.named_scope("list_one_wait"):
        list_one_copy.wait_recv()

    @pl.when(jnp.logical_not(at_end))
    def _():
        list_two_copy.start()
    with jax.named_scope("pass_far"):
        far_passes = [push_far(*target(move, (core + 1) % 2)) for move in flat_moves]

    @pl.when(core == 0)
    def _():
        push_far(*sibling)

    @pl.when(at_end & (core == 1))
    def _():
        pl.semaphore_signal(beside_sems.at[0], inc=1, device_id=sibling[0], device_id_type=MESH)

    @pl.when(at_end & (core == 0))
    def _():
        pl.semaphore_wait(beside_sems.at[0], 1)
        pl.semaphore_signal(across_sems.at[0], inc=1, device_id=opposite, device_id_type=MESH)
        pl.semaphore_wait(across_sems.at[0], 1)
        for copy in cross_copies:
            copy.start()
        list_two_copy.start()

    start_near()

    @pl.when(core == 1)
    def _():
        keep_far()
        with jax.named_scope("pass_far_wait"):
            await_level()
            for _, _, number in straight:
                level(number, pass_recv).wait_recv()

        @pl.when(at_end)
        def _():
            list_two_copy.start()
            with jax.named_scope("cross_late"):
                cross(True)

        @pl.when(jnp.logical_not(at_end))
        def _():
            with jax.named_scope("cross_late"):
                cross()

    with jax.named_scope("list_two_wait"):
        list_two_copy.wait_recv()
    with jax.named_scope("pass_near"):
        near_passes = [push_near(*one) for one in near_targets]
        keep_near()

    @pl.when(at_end & (core == 0))
    def _():
        pl.semaphore_signal(beside_sems.at[1], inc=1, device_id=sibling[0], device_id_type=MESH)

    @pl.when(at_end & (core == 1))
    def _():
        pl.semaphore_wait(beside_sems.at[1], 1)
        pl.semaphore_signal(across_sems.at[1], inc=1, device_id=opposite, device_id_type=MESH)
        pl.semaphore_wait(across_sems.at[1], 1)
        for copy in cross_copies:
            copy.start()


    spill_copy.wait()
    spill[...] = jnp.maximum(spill[...], spill_in[...])
    flag_copy = pltpu.make_async_copy(spill.at[2], starts.at[0], own_sems.at[0])
    flag_copy.start()
    flag_copy.wait()
    flag_ref[0, 0] = starts[0, starts.shape[1] - 1]
    def gather_near(land, at_layer, begun):
        limit = around * per_owner

        def one(column, _):
            value = total[column] if begun else blank
            for step in range(around):
                spot = near_table[at_layer * around + step, column] - at_layer * limit
                value = value + land[jnp.minimum(spot, limit)]
            total[column] = value
            return 0

        lax.fori_loop(0, local_blocks, one, 0)

    with jax.named_scope("near_own_wait"):
        for copy in near_copies:
            copy.wait_recv()
    gather_near(near_own, layer, False)
    with jax.named_scope("near_wait"):
        for copy in near_passes:
            copy.wait_recv()
    with jax.named_scope("near_sum"):
        gather_near(near_pass, 1 - layer, True)
    outs = []
    for index, copy in enumerate(cross_copies):
        with jax.named_scope(f"cross_wait{index}"):
            copy.wait_recv()
        part = pl.ds(index * chunk, chunk)
        total[part] = total[part] + crossed[part]
        out = pltpu.make_async_copy(total.at[part], out_hbm.at[part], out_sems.at[index])
        out.start()
        outs.append(out)
    sent = table_copies + far_copies + [list_one_copy, list_two_copy] + near_copies
    for copy in sent + far_passes + near_passes + cross_copies:
        copy.wait_send()

    @pl.when(core == 0)
    def _():
        sibling_pass(0, far_land).wait_send()

    for out in outs:
        out.wait()


def route_layers(owner, offset, block_row, sparse_blocks, panel_blocks, row_half, per_owner, first_list, list_slots):
    count = row_half * lax.axis_size("col")
    around = count // 2
    local_blocks, size, width = panel_blocks.shape
    half_slots = count * per_owner
    chunks = local_blocks // min(8, local_blocks)
    lanes = LANES
    made_slots = around * per_owner + half_slots + list_slots
    scalars = pl.BlockSpec(memory_space=pltpu.SMEM)
    anywhere = pl.BlockSpec(memory_space=pl.ANY)
    block = (size, width)
    dma = pltpu.SemaphoreType.DMA
    blocks = lambda number: pltpu.VMEM((number,) + block, jnp.float32)
    return pl.pallas_call(
        functools.partial(layer_kernel, row_half, per_owner, first_list),
        in_specs=[pl.BlockSpec(memory_space=pltpu.VMEM)] * 3 + [anywhere] * 2,
        out_specs=[anywhere, scalars],
        out_shape=[
            jax.ShapeDtypeStruct((local_blocks,) + block, jnp.float32),
            jax.ShapeDtypeStruct((1, 1), jnp.int32),
        ],
        scratch_shapes=[
            pltpu.VMEM(sparse_blocks.shape, jnp.float32),
            pltpu.VMEM(panel_blocks.shape, jnp.float32),
            blocks(around * per_owner + half_slots + list_slots),
            blocks(half_slots + 1),
            blocks(around * per_owner + 1),
            blocks(around * per_owner + 1),
            blocks(first_list),
            blocks(list_slots - first_list),
            blocks(local_blocks),
            blocks(local_blocks),
            blocks(local_blocks),
            pltpu.VMEM((count, TILE, lanes), jnp.int32),
            pltpu.VMEM((count, TILE, lanes), jnp.int32),
            pltpu.VMEM((-(-made_slots // lanes), lanes), jnp.int32),
            pltpu.SMEM((-(-made_slots // lanes), lanes), jnp.int32),
            pltpu.VMEM((TILE, lanes), jnp.int32),
            pltpu.VMEM((TILE, lanes), jnp.int32),
            pltpu.SMEM((count, lanes), jnp.int32),
            pltpu.SMEM((count, lanes), jnp.int32),
            pltpu.SMEM((count, lanes), jnp.int32),
            dma((count,)),
            dma((count,)),
            dma((around,)),
            dma((around,)),
            dma((2 * around,)),
            dma((2 * around,)),
            dma((2,)),
            dma((2,)),
            dma((count,)),
            dma((count,)),
            dma((chunks,)),
            dma((chunks,)),
            dma((2,)),
            dma((2,)),
            dma((5,)),
            dma((chunks,)),
            pltpu.SemaphoreType.REGULAR((2,)),
            pltpu.SemaphoreType.REGULAR((2,)),
        ],
        compiler_params=pltpu.CompilerParams(
            collective_id=1, has_side_effects=True, vmem_limit_bytes=VMEM_LIMIT
        ),
    )(owner, offset, block_row, sparse_blocks, panel_blocks)


def body(sparse_blocks, panel_rows, block_row, block_owner, block_offset):
    device_count = lax.axis_size("row") * lax.axis_size("col")
    half_count = device_count // 2
    slot_count, size, _ = sparse_blocks.shape
    width = panel_rows.shape[1]
    local_blocks = panel_rows.shape[0] // size
    per_owner = max(2, 2 * slot_count // device_count)
    half_slots = half_count * per_owner
    me = lax.axis_index(AXES)
    my_half = me // half_count
    row_half = lax.axis_size("row") // 2
    owner = block_owner[:, 0]
    panel_blocks = panel_rows.reshape(local_blocks, size, width)
    lanes = -(-max(local_blocks, LANES) // LANES) * LANES

    def whole():
        index = jnp.arange(slot_count, dtype=jnp.int32)
        key = block_offset * slot_count + index
        same = owner[:, None] == owner[None, :]
        earlier = same & (key[None, :] < key[:, None])
        order = jnp.sum(earlier.astype(jnp.int32), axis=1)
        again = jnp.any(earlier & (block_offset[None, :] == block_offset[:, None]), axis=1).astype(jnp.int32)
        far = (owner // half_count != my_half).astype(jnp.int32)
        group = far * half_count + owner % half_count
        landing = (me % half_count) * per_owner + order
        cell = (group[None, :] == jnp.arange(2 * half_count, dtype=jnp.int32)[:, None])[:, None, :] & (
            block_offset[None, :] == jnp.arange(lanes, dtype=jnp.int32)[:, None]
        )[None]
        table = jnp.max(jnp.where(cell, landing[None, None, :], -1), axis=2)
        table = jnp.where(table < 0, half_slots, table).reshape(2, half_count, 1, lanes)
        position = group * per_owner + order
        hit = position[None, :] == jnp.arange(2 * half_slots, dtype=jnp.int32)[:, None]
        pick = lambda value: jnp.max(jnp.where(hit, value[None, :], 0), axis=1)
        pair = table.transpose(1, 0, 2, 3)
        pair = jnp.broadcast_to(pair, (half_count, 2, TILE, lanes)).reshape(half_count, 2 * TILE, lanes)
        return route(
            pick(index), pick(block_row), pick(again), sparse_blocks, panel_blocks, pair, row_half, per_owner
        )

    lower = min(2, row_half)
    around = lower * lax.axis_size("col")
    if half_count != 2 * around or slot_count != LANES or not 8 <= local_blocks < LANES:
        return whole().reshape(local_blocks * size, width)

    first_list = around // 2 * per_owner
    list_slots = max(slot_count // 2, first_list + 8)
    as_row = lambda value: value.reshape(1, slot_count)
    total, flags = route_layers(
        as_row(block_owner),
        as_row(block_offset),
        as_row(block_row),
        sparse_blocks,
        panel_blocks,
        row_half,
        per_owner,
        first_list,
        list_slots,
    )
    total = lax.cond(flags[0, 0] > list_slots, whole, lambda: total)
    return total.reshape(local_blocks * size, width)


def solution(mesh):
    placed = (
        P(AXES, None, None),
        P(AXES, None),
        P(AXES),
        P(AXES, None),
        P(AXES),
    )
    return jax.shard_map(
        body, mesh=mesh, in_specs=placed, out_specs=P(AXES, None), check_vma=False
    )
```

```python
import functools

import jax
import jax.numpy as jnp
from jax import lax
from jax.experimental import pallas as pl
from jax.experimental.pallas import tpu as pltpu
from jax.sharding import PartitionSpec as P

AXES = ("row", "col")
VMEM_LIMIT = 67_000_000
LANES = 128
TILE = 8
MESH = pl.DeviceIdType.MESH


def split_parts(value):
    high = value.astype(jnp.bfloat16)
    low = (value - high.astype(jnp.float32)).astype(jnp.bfloat16)
    return high, low


def block_product(block, panel):
    block_high, block_low = split_parts(block)
    panel_high, panel_low = split_parts(panel)
    dims = (((0,), (0,)), ((), ()))
    dot = functools.partial(lax.dot_general, dimension_numbers=dims, preferred_element_type=jnp.float32)
    return dot(
        jnp.concatenate([block_high, block_low], axis=0),
        jnp.concatenate([panel_high, panel_high], axis=0),
    ) + dot(block_high, panel_low)


def peers_of(upper, lower, outer):
    moves = [
        (a, b, c) for a in range(upper) for b in range(lower) for c in range(outer) if (a, b, c) != (0, 0, 0)
    ]
    single = [move for move in moves if sum(digit > 0 for digit in move) == 1]
    double = [move for move in moves if sum(digit > 0 for digit in move) == 2]
    zeros = lambda move: tuple(digit == 0 for digit in move)
    order = sorted(single, key=zeros)
    opposite = sorted(double, key=lambda move: tuple(digit > 0 for digit in move))
    pairs = list(zip(order, opposite))
    first = [one for one, _ in pairs] + [other for _, other in pairs]
    second = [other for _, other in pairs] + [one for one, _ in pairs]
    rest = [move for move in moves if move not in first]
    return first + rest, second + rest


def route_kernel(
    row_half,
    per_owner,
    source_ref,
    panel_at_ref,
    keep_ref,
    sparse_hbm,
    panel_hbm,
    table_hbm,
    out_hbm,
    sparse,
    panel,
    products,
    far_land,
    near_land,
    sums,
    crossed,
    total,
    tables,
    near_table,
    far_table,
    data_send,
    data_recv,
    table_send,
    table_recv,
    cross_send,
    cross_recv,
    load_sems,
    own_sems,
    out_sems,
):
    row, col = lax.axis_index("row"), lax.axis_index("col")
    row_count, col_count = lax.axis_size("row"), lax.axis_size("col")
    half, inner = row // row_half, row % row_half
    outer, core = col // 2, col % 2
    lower = min(2, row_half)
    mine = inner * col_count + col
    count = row_half * col_count
    half_slots = count * per_owner
    upper_count, outer_count = row_half // lower, col_count // 2
    local_blocks = total.shape[0]
    chunk = min(8, local_blocks)
    chunks = local_blocks // chunk

    loads = [
        pltpu.make_async_copy(sparse_hbm, sparse, load_sems.at[0]),
        pltpu.make_async_copy(panel_hbm, panel, load_sems.at[1]),
    ]
    for load in loads:
        load.start()
    blank = jnp.zeros(far_land.shape[1:], jnp.float32)
    far_land[half_slots] = blank
    near_land[half_slots] = blank

    def target(move_pair, flip):
        one, other = move_pair
        a, b, c = (x + core * (y - x) for x, y in zip(one, other))
        there = (inner // lower + a) % upper_count * lower + (inner % lower + b) % lower
        beside = (outer + c) % outer_count * 2 + (core + flip) % 2
        number = ((a * lower + b) * outer_count + c) * 2 + flip
        return (half * row_half + there, beside), there * col_count + beside, number

    firsts, seconds = peers_of(upper_count, lower, outer_count)
    moves = list(zip(firsts, seconds))
    still = ((0, 0, 0), (0, 0, 0))
    targets = [target(move, (core + phase) % 2) for phase in range(2) for move in moves]
    targets.append(target(still, 1))
    opposite = ((row + row_half) % row_count, col)

    barrier = pltpu.get_barrier_semaphore()
    for device, _, _ in targets:
        pl.semaphore_signal(barrier, inc=1, device_id=device, device_id_type=MESH)
    pl.semaphore_signal(barrier, inc=1, device_id=opposite, device_id_type=MESH)
    pl.semaphore_wait(barrier, len(targets) + 1)

    def remote(source, destination, send_sem, recv_sem, device):
        copy = pltpu.make_async_remote_copy(
            src_ref=source,
            dst_ref=destination,
            send_sem=send_sem,
            recv_sem=recv_sem,
            device_id=device,
            device_id_type=MESH,
        )
        copy.start()
        return copy

    table_copies = [
        remote(table_hbm.at[place], tables.at[mine], table_send.at[number], table_recv.at[number], device)
        for device, place, number in targets
    ]
    own_table = pltpu.make_async_copy(table_hbm.at[mine], tables.at[mine], own_sems.at[0])
    own_table.start()
    for load in loads:
        load.wait()

    unit = min(4, per_owner)

    def fill(base, place, destination, at):
        first = base + place * per_owner

        def some(step, _):
            for k in range(unit):
                slot = step * unit + k
                source = source_ref[first + slot]
                product = block_product(sparse[source], panel[panel_at_ref[first + slot]])
                before = destination[at + jnp.maximum(slot - 1, 0)]
                product = product + jnp.where(keep_ref[first + slot] > 0, before, 0.0)
                destination[at + slot] = product
            return 0

        lax.fori_loop(0, per_owner // unit, some, 0)

    def spread(base, land, shift):
        copies = []
        for device, place, number in targets:
            at = base + place * per_owner
            fill(base, place, products, at)
            copies.append(
                remote(
                    products.at[pl.ds(at, per_owner)],
                    land.at[pl.ds(mine * per_owner, per_owner)],
                    data_send.at[shift + number],
                    data_recv.at[shift + number],
                    device,
                )
            )
        fill(base, mine, land, mine * per_owner)
        return copies

    far_copies = spread(half_slots, far_land, count)
    near_copies = spread(0, near_land, 0)

    own_table.wait()
    for copy in table_copies:
        copy.wait_recv()
    lookups = [
        pltpu.make_async_copy(tables.at[:, 0, :], near_table, own_sems.at[1]),
        pltpu.make_async_copy(tables.at[:, TILE, :], far_table, own_sems.at[2]),
    ]
    for lookup in lookups:
        lookup.start()
    for lookup in lookups:
        lookup.wait()

    def reduce(land, table, destination, first, number):
        def one(step, _):
            column = first + step
            value = land[table[0, column]]
            for origin in range(1, count):
                value = value + land[table[origin, column]]
            destination[column] = value
            return 0

        lax.fori_loop(0, number, one, 0)

    for copy in far_copies:
        copy.wait_recv()
    cross_copies = []
    for index in range(chunks):
        reduce(far_land, far_table, sums, index * chunk, chunk)
        part = pl.ds(index * chunk, chunk)
        cross_copies.append(
            remote(sums.at[part], crossed.at[part], cross_send.at[index], cross_recv.at[index], opposite)
        )
    for copy in near_copies:
        copy.wait_recv()
    reduce(near_land, near_table, total, 0, local_blocks)
    outs = []
    for index, copy in enumerate(cross_copies):
        copy.wait_recv()
        part = pl.ds(index * chunk, chunk)
        total[part] = total[part] + crossed[part]
        out = pltpu.make_async_copy(total.at[part], out_hbm.at[part], out_sems.at[index])
        out.start()
        outs.append(out)
    for copy in table_copies + far_copies + near_copies + cross_copies:
        copy.wait_send()
    for out in outs:
        out.wait()


def route(source, panel_at, keep, sparse_blocks, panel_blocks, table, row_half, per_owner):
    count = row_half * lax.axis_size("col")
    local_blocks, size, width = panel_blocks.shape
    half_slots = count * per_owner
    chunks = local_blocks // min(8, local_blocks)
    lanes = table.shape[-1]
    scalars = pl.BlockSpec(memory_space=pltpu.SMEM)
    anywhere = pl.BlockSpec(memory_space=pl.ANY)
    block = (size, width)
    dma = pltpu.SemaphoreType.DMA
    return pl.pallas_call(
        functools.partial(route_kernel, row_half, per_owner),
        in_specs=[scalars] * 3 + [anywhere] * 3,
        out_specs=anywhere,
        out_shape=jax.ShapeDtypeStruct((local_blocks,) + block, jnp.float32),
        scratch_shapes=[
            pltpu.VMEM(sparse_blocks.shape, jnp.float32),
            pltpu.VMEM(panel_blocks.shape, jnp.float32),
            pltpu.VMEM((2 * half_slots,) + block, jnp.float32),
            pltpu.VMEM((half_slots + 1,) + block, jnp.float32),
            pltpu.VMEM((half_slots + 1,) + block, jnp.float32),
            pltpu.VMEM((local_blocks,) + block, jnp.float32),
            pltpu.VMEM((local_blocks,) + block, jnp.float32),
            pltpu.VMEM((local_blocks,) + block, jnp.float32),
            pltpu.VMEM((count, 2 * TILE, lanes), jnp.int32),
            pltpu.SMEM((count, lanes), jnp.int32),
            pltpu.SMEM((count, lanes), jnp.int32),
            dma((2 * count,)),
            dma((2 * count,)),
            dma((count,)),
            dma((count,)),
            dma((chunks,)),
            dma((chunks,)),
            dma((2,)),
            dma((3,)),
            dma((chunks,)),
        ],
        compiler_params=pltpu.CompilerParams(
            collective_id=0, has_side_effects=True, vmem_limit_bytes=VMEM_LIMIT
        ),
    )(source, panel_at, keep, sparse_blocks, panel_blocks, table)


def prepare(owner_ref, offset_ref, row_ref, made, slots_made, half, mine, per_owner, count, around, local_blocks, list_slots):
    slots = owner_ref.shape[1]
    items = (owner_ref[...] * local_blocks + offset_ref[...]) * local_blocks + row_ref[...]
    across = jnp.broadcast_to(items, (slots, slots))
    down = jnp.transpose(across)
    lane = lax.broadcasted_iota(jnp.int32, (slots, LANES), 1)
    item = lax.broadcasted_iota(jnp.int32, (slots, LANES), 0)
    half_slots = count * per_owner

    def parts(packed):
        offset = packed // local_blocks % local_blocks
        owner = packed // (local_blocks * local_blocks)
        far = owner // count != half
        place = jnp.where(far, (owner + around) % count, owner % count)
        flat = place % around
        listed = (place // around != mine // around) & (jnp.logical_not(far) | (flat % 2 == 1))
        list_group = jnp.where(listed, jnp.where(far, flat // 2, around // 2 + flat), LANES)
        return owner, offset, far, place, flat, listed, list_group

    owner_r, offset_r, _, _, _, _, list_group_r = parts(across)
    owner_c, offset_c, far_c, place_c, flat_c, listed_c, list_group_c = parts(down)
    key_r, key_c = offset_r * slots + lane, offset_c * slots + item
    earlier = (owner_r == owner_c) & (key_r < key_c)
    total = lambda mask, value: jnp.sum(jnp.where(mask, value, 0), axis=1, keepdims=True)
    ranked = total(earlier, jnp.where(offset_r == offset_c, slots + 1, 1))
    order, again = jnp.minimum(ranked % slots, per_owner - 1), jnp.minimum(ranked // slots, 1)
    ahead = total(list_group_r < list_group_c, 1)
    position = jnp.where(
        listed_c,
        around * per_owner + half_slots + ahead + order,
        jnp.where(far_c, around * per_owner + place_c * per_owner + order, flat_c * per_owner + order),
    )
    packed = (item * local_blocks + down % local_blocks) * 2 + again
    for block in range(slots_made.shape[0]):
        picked = jnp.max(jnp.where(position == lane + block * LANES, packed, 0), axis=0, keepdims=True)
        slots_made[pl.ds(block, 1), :] = picked
    starts = jnp.sum((list_group_c < lane).astype(jnp.int32), axis=0, keepdims=True)
    landing = jnp.where(offset_c == lane, mine * per_owner + order, -1)
    kind = lax.broadcasted_iota(jnp.int32, (TILE, LANES), 0)

    def table(far, index):
        own = (far_c == far) & (place_c == index)
        best = jnp.max(jnp.where(own, landing, -1), axis=0, keepdims=True)
        return jnp.where(best < 0, half_slots, best)

    for index in range(count):
        near, away = table(False, index), table(True, index)
        made[index] = jnp.where(kind == 0, near, jnp.where(kind == 1, away, starts))


def layer_kernel(
    row_half,
    per_owner,
    first_list,
    owner_ref,
    offset_ref,
    row_ref,
    sparse_hbm,
    panel_hbm,
    out_hbm,
    flag_ref,
    sparse,
    panel,
    products,
    far_land,
    near_own,
    near_pass,
    list_one,
    list_two,
    sums,
    crossed,
    total,
    tables,
    made,
    slots_made,
    slot_ref,
    spill,
    spill_in,
    near_table,
    far_table,
    starts,
    far_send,
    far_recv,
    near_send,
    near_recv,
    pass_send,
    pass_recv,
    list_send,
    list_recv,
    table_send,
    table_recv,
    cross_send,
    cross_recv,
    spill_sems,
    load_sems,
    own_sems,
    out_sems,
    beside_sems,
    across_sems,
):
    row, col = lax.axis_index("row"), lax.axis_index("col")
    col_count = lax.axis_size("col")
    half, inner = row // row_half, row % row_half
    outer, core = col // 2, col % 2
    lower = min(2, row_half)
    layer, beside_x = inner // lower, inner % lower
    mine = inner * col_count + col
    count = row_half * col_count
    around = lower * col_count
    half_slots = count * per_owner
    outer_count = col_count // 2
    rows_of_panel = panel.shape[0]
    local_blocks = total.shape[0]
    chunk = min(8, local_blocks)
    chunks = local_blocks // chunk
    second_list = list_two.shape[0]
    near_base, far_base, list_base = 0, around * per_owner, around * per_owner + half_slots

    loads = [
        pltpu.make_async_copy(sparse_hbm, sparse, load_sems.at[0]),
        pltpu.make_async_copy(panel_hbm, panel, load_sems.at[1]),
    ]
    for load in loads:
        load.start()
    blank = jnp.zeros(far_land.shape[1:], jnp.float32)
    far_land[half_slots] = blank
    near_own[around * per_owner] = blank
    near_pass[around * per_owner] = blank

    def target(move_pair, flip):
        one, other = move_pair
        a, b, c = (x + core * (y - x) for x, y in zip(one, other))
        there = (layer + a) % 2 * lower + (beside_x + b) % lower
        beside = (outer + c) % outer_count * 2 + (core + flip) % 2
        number = ((a * lower + b) * outer_count + c) * 2 + flip
        return (half * row_half + there, beside), there * col_count + beside, number

    firsts, seconds = peers_of(2, lower, outer_count)
    moves = list(zip(firsts, seconds))
    flat = [move for move in firsts if move[0] == 0]
    flat_moves = list(zip(flat, sorted(flat, key=lambda move: (sum(move), move[1]))))
    still = ((0, 0, 0), (0, 0, 0))
    sibling = target(still, 1)
    partner_inner = (layer + 1) % 2 * lower + beside_x
    partner, partner_place = (half * row_half + partner_inner, col), partner_inner * col_count + col
    opposite = ((1 - half) * row_half + (1 - layer) * lower + beside_x, col)

    everyone = [target(move, (core + phase) % 2) for phase in range(2) for move in moves] + [sibling]
    barrier = pltpu.get_barrier_semaphore()
    for device, _, _ in everyone:
        pl.semaphore_signal(barrier, inc=1, device_id=device, device_id_type=MESH)
    pl.semaphore_signal(barrier, inc=1, device_id=opposite, device_id_type=MESH)

    with jax.named_scope("prepare"):
        prepare(
            owner_ref,
            offset_ref,
            row_ref,
            made,
            slots_made,
            half,
            mine,
            per_owner,
            count,
            around,
            local_blocks,
            first_list + second_list,
        )
        slot_copy = pltpu.make_async_copy(slots_made, slot_ref, own_sems.at[4])
        slot_copy.start()
    with jax.named_scope("barrier"):
        pl.semaphore_wait(barrier, len(everyone) + 1)

    def remote(source, destination, send_sem, recv_sem, device):
        return pltpu.make_async_remote_copy(
            src_ref=source,
            dst_ref=destination,
            send_sem=send_sem,
            recv_sem=recv_sem,
            device_id=device,
            device_id_type=MESH,
        )

    def begin(copy):
        copy.start()
        return copy

    table_copies = [
        begin(remote(made.at[place], tables.at[mine], table_send.at[number], table_recv.at[number], device))
        for device, place, number in everyone
    ]
    own_table = pltpu.make_async_copy(made.at[mine], tables.at[mine], own_sems.at[0])
    own_table.start()
    slot_copy.wait()
    with jax.named_scope("load_wait"):
        for load in loads:
            load.wait()

    def fill(base, slots, destination, at, lead=0):
        unit = min(4, slots)

        def some(step, _):
            for k in range(unit):
                slot = step * unit + k
                packed = slot_ref[(base + slot) // LANES, (base + slot) % LANES]
                source, panel_at = packed // (2 * rows_of_panel), packed // 2 % rows_of_panel
                product = block_product(sparse[source], panel[panel_at])
                before = destination[at + jnp.maximum(slot - 1, -lead)]
                destination[at + slot] = product + jnp.where(packed % 2 > 0, before, 0.0)
            return 0

        lax.fori_loop(0, slots // unit, some, 0)

    def direct(base, index, land, spot, send, recv, number, device, later=False):
        at = base + index * per_owner
        copy = remote(
            products.at[pl.ds(at, per_owner)],
            land.at[pl.ds(spot * per_owner, per_owner)],
            send.at[number],
            recv.at[number],
            device,
        )

        fill(at, per_owner, products, at)
        if not later:
            copy.start()
        return copy

    def send_far(device, place, number):
        return direct(far_base, place, far_land, mine, far_send, far_recv, number, device)

    def send_near(device, place, number):
        return direct(near_base, place % around, near_own, mine % around, near_send, near_recv, number, device, True)

    def send_list(first, land, index):
        slots = land.shape[0]
        fill(list_base + first, slots, products, list_base + first, min(first, 1))
        return remote(
            products.at[pl.ds(list_base + first, slots)], land, list_send.at[index], list_recv.at[index], partner
        )

    with jax.named_scope("far_first"):
        far_copies = [send_far(*target(move, core)) for move in sorted(moves, key=lambda pair: -pair[0][0] - pair[1][0])]
    with jax.named_scope("list_one"):
        list_one_copy = begin(send_list(0, list_one, 0))
    with jax.named_scope("far_second"):
        far_copies += [send_far(*target(move, (core + 1) % 2)) for move in flat_moves]
        far_copies.append(send_far(*sibling))
        fill(far_base + mine * per_owner, per_owner, far_land, mine * per_owner)
    with jax.named_scope("list_two"):
        list_two_copy = send_list(first_list, list_two, 1)

    at_end = layer == half

    near_targets = [target(move, (core + phase) % 2) for phase in range(2) for move in flat_moves] + [sibling]
    with jax.named_scope("near_own"):
        near_copies = [send_near(*one) for one in near_targets]
        fill(near_base + mine % around * per_owner, per_owner, near_own, mine % around * per_owner)

    def start_near():
        for copy in near_copies:
            copy.start()

    with jax.named_scope("table_wait"):
        own_table.wait()
        for copy in table_copies:
            copy.wait_recv()
    lookups = [
        pltpu.make_async_copy(tables.at[:, 0, :], near_table, own_sems.at[1]),
        pltpu.make_async_copy(tables.at[:, 1, :], far_table, own_sems.at[2]),
        pltpu.make_async_copy(tables.at[:, 2, :], starts, own_sems.at[3]),
    ]
    for lookup in lookups:
        lookup.start()
    worst = tables[0]
    for origin in range(1, count):
        worst = jnp.maximum(worst, tables[origin])
    spill[...] = worst
    spill_copy = begin(remote(spill, spill_in, spill_sems.at[0], spill_sems.at[1], opposite))
    for lookup in lookups:
        lookup.wait()

    def reduce(land, table, destination, first, number):
        def one(step, _):
            column = first + step
            value = land[table[0, column]]
            for origin in range(1, count):
                value = value + land[table[origin, column]]
            destination[column] = value
            return 0

        lax.fori_loop(0, number, one, 0)

    cross_copies = [
        remote(
            sums.at[pl.ds(index * chunk, chunk)],
            crossed.at[pl.ds(index * chunk, chunk)],
            cross_send.at[index],
            cross_recv.at[index],
            opposite,
        )
        for index in range(chunks)
    ]

    def cross(held=False):
        for index in range(chunks):
            reduce(far_land, far_table, sums, index * chunk, chunk)
            if not held:
                cross_copies[index].start()

    straight = [target(move, (core + phase) % 2) for phase in range(2) for move in flat_moves] + [sibling]
    level = lambda number, recv: remote(
        products.at[pl.ds(0, per_owner)],
        far_land.at[pl.ds(mine * per_owner, per_owner)],
        far_send.at[0],
        recv.at[number],
        partner,
    )

    def await_level():
        for _, _, number in straight:
            level(number, far_recv).wait_recv()

    @pl.when(core == 0)
    def _():
        with jax.named_scope("far_wait"):
            await_level()
            for number in range(around, count):
                level(number, far_recv).wait_recv()
        @pl.when(at_end)
        def _():
            with jax.named_scope("cross_early"):
                cross(True)

        @pl.when(jnp.logical_not(at_end))
        def _():
            with jax.named_scope("cross_early"):
                cross()

    def relay(index, starting, land, spot, shift, both):
        def pull(place, destination, at):
            start = starts[partner_place, starting(place % around)]

            def one(k, _):
                where = start + k
                value = list_one[jnp.minimum(where, first_list - 1)]
                if both:
                    other = list_two[jnp.clip(where - first_list, 0, second_list - 1)]
                    value = jnp.where(where < first_list, value, other)
                destination[at + k] = value
                return 0

            lax.fori_loop(0, per_owner, one, 0)

        def push(device, place, number):
            at = shift + place % around * per_owner
            pull(place, sparse, at)
            return begin(
                remote(
                    sparse.at[pl.ds(at, per_owner)],
                    land.at[pl.ds(spot * per_owner, per_owner)],
                    pass_send.at[index * around + number],
                    pass_recv.at[index * around + number],
                    device,
                )
            )

        def keep():
            pull(mine, land, spot * per_owner)

        return push, keep

    push_far, keep_far = relay(0, lambda place: place // 2, far_land, partner_place, 0, False)
    push_near, keep_near = relay(
        1, lambda place: around // 2 + place, near_pass, mine % around, around * per_owner, True
    )
    sibling_pass = lambda index, land: remote(
        sparse.at[pl.ds(0, per_owner)],
        land.at[pl.ds(partner_place * per_owner, per_owner)],
        pass_send.at[index * around + 1],
        pass_recv.at[index * around + 1],
        sibling[0],
    )

    with jax.named_scope("list_one_wait"):
        list_one_copy.wait_recv()

    in_turn = jnp.logical_not(at_end) & (core == 0)

    @pl.when(in_turn)
    def _():
        list_two_copy.start()
    with jax.named_scope("pass_far"):
        far_passes = [push_far(*target(move, (core + 1) % 2)) for move in flat_moves]

    @pl.when(core == 0)
    def _():
        push_far(*sibling)

    @pl.when(at_end & (core == 1))
    def _():
        pl.semaphore_signal(beside_sems.at[0], inc=1, device_id=sibling[0], device_id_type=MESH)

    @pl.when(at_end & (core == 0))
    def _():
        pl.semaphore_wait(beside_sems.at[0], 1)
        pl.semaphore_signal(across_sems.at[0], inc=1, device_id=opposite, device_id_type=MESH)
        pl.semaphore_wait(across_sems.at[0], 1)
        for copy in cross_copies:
            copy.start()
        list_two_copy.start()

    start_near()

    @pl.when(core == 1)
    def _():
        keep_far()
        with jax.named_scope("pass_far_wait"):
            await_level()
            for _, _, number in straight:
                level(number, pass_recv).wait_recv()

        @pl.when(at_end)
        def _():
            list_two_copy.start()
            with jax.named_scope("cross_late"):
                cross(True)

        @pl.when(jnp.logical_not(at_end))
        def _():
            with jax.named_scope("cross_late"):
                cross()

    @pl.when(in_turn)
    def _():
        list_two_copy.wait_send()
        pl.semaphore_signal(beside_sems.at[0], inc=1, device_id=sibling[0], device_id_type=MESH)

    @pl.when(jnp.logical_not(at_end) & (core == 1))
    def _():
        pl.semaphore_wait(beside_sems.at[0], 1)
        list_two_copy.start()

    with jax.named_scope("list_two_wait"):
        list_two_copy.wait_recv()
    @pl.when(at_end & (core == 0))
    def _():
        pl.semaphore_signal(beside_sems.at[1], inc=1, device_id=sibling[0], device_id_type=MESH)

    @pl.when(at_end & (core == 1))
    def _():
        pl.semaphore_wait(beside_sems.at[1], 1)
        pl.semaphore_signal(across_sems.at[1], inc=1, device_id=opposite, device_id_type=MESH)
        pl.semaphore_wait(across_sems.at[1], 1)
        for copy in cross_copies:
            copy.start()

    with jax.named_scope("pass_near"):
        near_passes = [push_near(*one) for one in near_targets]
        keep_near()


    spill_copy.wait()
    spill[...] = jnp.maximum(spill[...], spill_in[...])
    flag_copy = pltpu.make_async_copy(spill.at[2], starts.at[0], own_sems.at[0])
    flag_copy.start()
    flag_copy.wait()
    flag_ref[0, 0] = starts[0, starts.shape[1] - 1]
    def gather_near(land, at_layer, begun):
        limit = around * per_owner

        def one(column, _):
            value = total[column] if begun else blank
            for step in range(around):
                spot = near_table[at_layer * around + step, column] - at_layer * limit
                value = value + land[jnp.minimum(spot, limit)]
            total[column] = value
            return 0

        lax.fori_loop(0, local_blocks, one, 0)

    with jax.named_scope("near_own_wait"):
        for copy in near_copies:
            copy.wait_recv()
    gather_near(near_own, layer, False)
    with jax.named_scope("near_wait"):
        for copy in near_passes:
            copy.wait_recv()
    with jax.named_scope("near_sum"):
        gather_near(near_pass, 1 - layer, True)
    outs = []
    for index, copy in enumerate(cross_copies):
        with jax.named_scope(f"cross_wait{index}"):
            copy.wait_recv()
        part = pl.ds(index * chunk, chunk)
        total[part] = total[part] + crossed[part]
        out = pltpu.make_async_copy(total.at[part], out_hbm.at[part], out_sems.at[index])
        out.start()
        outs.append(out)
    sent = table_copies + far_copies + [list_one_copy] + near_copies
    for copy in sent + far_passes + near_passes + cross_copies:
        copy.wait_send()

    @pl.when(jnp.logical_not(in_turn))
    def _():
        list_two_copy.wait_send()

    @pl.when(core == 0)
    def _():
        sibling_pass(0, far_land).wait_send()

    for out in outs:
        out.wait()


def route_layers(owner, offset, block_row, sparse_blocks, panel_blocks, row_half, per_owner, first_list, list_slots):
    count = row_half * lax.axis_size("col")
    around = count // 2
    local_blocks, size, width = panel_blocks.shape
    half_slots = count * per_owner
    chunks = local_blocks // min(8, local_blocks)
    lanes = LANES
    made_slots = around * per_owner + half_slots + list_slots
    scalars = pl.BlockSpec(memory_space=pltpu.SMEM)
    anywhere = pl.BlockSpec(memory_space=pl.ANY)
    block = (size, width)
    dma = pltpu.SemaphoreType.DMA
    blocks = lambda number: pltpu.VMEM((number,) + block, jnp.float32)
    return pl.pallas_call(
        functools.partial(layer_kernel, row_half, per_owner, first_list),
        in_specs=[pl.BlockSpec(memory_space=pltpu.VMEM)] * 3 + [anywhere] * 2,
        out_specs=[anywhere, scalars],
        out_shape=[
            jax.ShapeDtypeStruct((local_blocks,) + block, jnp.float32),
            jax.ShapeDtypeStruct((1, 1), jnp.int32),
        ],
        scratch_shapes=[
            pltpu.VMEM(sparse_blocks.shape, jnp.float32),
            pltpu.VMEM(panel_blocks.shape, jnp.float32),
            blocks(around * per_owner + half_slots + list_slots),
            blocks(half_slots + 1),
            blocks(around * per_owner + 1),
            blocks(around * per_owner + 1),
            blocks(first_list),
            blocks(list_slots - first_list),
            blocks(local_blocks),
            blocks(local_blocks),
            blocks(local_blocks),
            pltpu.VMEM((count, TILE, lanes), jnp.int32),
            pltpu.VMEM((count, TILE, lanes), jnp.int32),
            pltpu.VMEM((-(-made_slots // lanes), lanes), jnp.int32),
            pltpu.SMEM((-(-made_slots // lanes), lanes), jnp.int32),
            pltpu.VMEM((TILE, lanes), jnp.int32),
            pltpu.VMEM((TILE, lanes), jnp.int32),
            pltpu.SMEM((count, lanes), jnp.int32),
            pltpu.SMEM((count, lanes), jnp.int32),
            pltpu.SMEM((count, lanes), jnp.int32),
            dma((count,)),
            dma((count,)),
            dma((around,)),
            dma((around,)),
            dma((2 * around,)),
            dma((2 * around,)),
            dma((2,)),
            dma((2,)),
            dma((count,)),
            dma((count,)),
            dma((chunks,)),
            dma((chunks,)),
            dma((2,)),
            dma((2,)),
            dma((5,)),
            dma((chunks,)),
            pltpu.SemaphoreType.REGULAR((2,)),
            pltpu.SemaphoreType.REGULAR((2,)),
        ],
        compiler_params=pltpu.CompilerParams(
            collective_id=1, has_side_effects=True, vmem_limit_bytes=VMEM_LIMIT
        ),
    )(owner, offset, block_row, sparse_blocks, panel_blocks)


def body(sparse_blocks, panel_rows, block_row, block_owner, block_offset):
    device_count = lax.axis_size("row") * lax.axis_size("col")
    half_count = device_count // 2
    slot_count, size, _ = sparse_blocks.shape
    width = panel_rows.shape[1]
    local_blocks = panel_rows.shape[0] // size
    per_owner = max(2, 2 * slot_count // device_count)
    half_slots = half_count * per_owner
    me = lax.axis_index(AXES)
    my_half = me // half_count
    row_half = lax.axis_size("row") // 2
    owner = block_owner[:, 0]
    panel_blocks = panel_rows.reshape(local_blocks, size, width)
    lanes = -(-max(local_blocks, LANES) // LANES) * LANES

    def whole():
        index = jnp.arange(slot_count, dtype=jnp.int32)
        key = block_offset * slot_count + index
        same = owner[:, None] == owner[None, :]
        earlier = same & (key[None, :] < key[:, None])
        order = jnp.sum(earlier.astype(jnp.int32), axis=1)
        again = jnp.any(earlier & (block_offset[None, :] == block_offset[:, None]), axis=1).astype(jnp.int32)
        far = (owner // half_count != my_half).astype(jnp.int32)
        group = far * half_count + owner % half_count
        landing = (me % half_count) * per_owner + order
        cell = (group[None, :] == jnp.arange(2 * half_count, dtype=jnp.int32)[:, None])[:, None, :] & (
            block_offset[None, :] == jnp.arange(lanes, dtype=jnp.int32)[:, None]
        )[None]
        table = jnp.max(jnp.where(cell, landing[None, None, :], -1), axis=2)
        table = jnp.where(table < 0, half_slots, table).reshape(2, half_count, 1, lanes)
        position = group * per_owner + order
        hit = position[None, :] == jnp.arange(2 * half_slots, dtype=jnp.int32)[:, None]
        pick = lambda value: jnp.max(jnp.where(hit, value[None, :], 0), axis=1)
        pair = table.transpose(1, 0, 2, 3)
        pair = jnp.broadcast_to(pair, (half_count, 2, TILE, lanes)).reshape(half_count, 2 * TILE, lanes)
        return route(
            pick(index), pick(block_row), pick(again), sparse_blocks, panel_blocks, pair, row_half, per_owner
        )

    lower = min(2, row_half)
    around = lower * lax.axis_size("col")
    if half_count != 2 * around or slot_count != LANES or not 8 <= local_blocks < LANES:
        return whole().reshape(local_blocks * size, width)

    first_list = around // 2 * per_owner
    list_slots = max(slot_count // 2, first_list + 8)
    as_row = lambda value: value.reshape(1, slot_count)
    total, flags = route_layers(
        as_row(block_owner),
        as_row(block_offset),
        as_row(block_row),
        sparse_blocks,
        panel_blocks,
        row_half,
        per_owner,
        first_list,
        list_slots,
    )
    total = lax.cond(flags[0, 0] > list_slots, whole, lambda: total)
    return total.reshape(local_blocks * size, width)


def solution(mesh):
    placed = (
        P(AXES, None, None),
        P(AXES, None),
        P(AXES),
        P(AXES, None),
        P(AXES),
    )
    return jax.shard_map(
        body, mesh=mesh, in_specs=placed, out_specs=P(AXES, None), check_vma=False
    )
```
